32 devices in a mesh: ctx: 8 (over z, y), tp: 4 (over x, core).
Axes of the slice: x: 2, y: 2, z: 4, core: 2. Of those that a mesh axis runs over, the one named last changes fastest.
Arguments:
- queries: bfloat16 [2048, 64, 128], P('ctx', 'tp'), may hold values from -48 to 48
- keys: bfloat16 [2048, 8, 128], P('ctx', 'tp'), may hold values from -3 to 3
- values: bfloat16 [2048, 8, 128], P('ctx', 'tp'), may hold values from -6 to 6
- segment_ids: int32 [2048], P('ctx'), may hold values from 0 to 7, never falling along the last dimension, each value on 1 to 1280 neighbouring positions
Outputs:
- attended: bfloat16 [2048, 8192], P(('ctx', 'tp'))
The draws below stay inside these ranges and needn't reach their ends.
Inputs may be any that keep to these rules, and one draw needn't show every extreme that they name: `segment_ids`: ids never fall along the tokens; each document holds 1 to 1280 tokens, and one holds exactly 1280.
All inputs are finite; a program needn't handle non-finite values.
Results may differ from the reference program's by a relative error of at most 0.003.
Values may be sent and summed in bfloat16 or wider, within the bound.
A program may use at most 64 MiB of HBM per device.

```python
import math
import jax
import jax.numpy as jnp
import numpy as np
from jax import lax

QUERY_HEADS = 64
KEY_VALUE_HEADS = 8
HEAD_SIZE = 128
DOCS = 8
PACK_TOKENS = 2048
MOST = 1280


def paired_draw(key):
    base = jax.random.fold_in(key, 4242)
    key_random_keys, key_query = jax.random.split(base, 2)
    keys = jnp.clip(jax.random.normal(key_random_keys, (PACK_TOKENS, KEY_VALUE_HEADS, HEAD_SIZE), jnp.float32), -3.0, 3.0)
    queries = jnp.clip(2.5 * jax.random.normal(key_query, (PACK_TOKENS, QUERY_HEADS, HEAD_SIZE), jnp.float32), -12.0, 12.0)
    return (queries.astype(jnp.bfloat16), keys.astype(jnp.bfloat16))


def draw_queries(key, part):
    return paired_draw(key)[0]


def draw_keys(key, part):
    return paired_draw(key)[1]


def shard_levels(own_key, extent, cuts, least, high):
    loudness, own = 1.0, jax.random.fold_in(own_key, 6)
    for position, shards_of in cuts:
        heights = jnp.exp(jax.random.uniform(jax.random.fold_in(own, position), (shards_of,), jnp.float32, least / len(cuts), high / len(cuts)))
        loudness = loudness * jnp.repeat(heights, extent[position] // shards_of).reshape([-1 if axis == position else 1 for axis in range(len(extent))])
    return loudness


def length_profile(count, total, most, lean):
    weights = [(1 << 20) // math.isqrt(standing ** lean) + 1 for standing in range(2, count + 1)]
    spare, given = total - most - (count - 1), [1] * (count - 1)
    while spare > 0:
        free = [i for i in range(count - 1) if given[i] < most]
        mass, remaining = sum([weights[i] for i in free]), spare
        for i in free:
            addition = min(most - given[i], max(1, remaining * weights[i] // mass), spare)
            given[i] = given[i] + addition
            spare = spare - addition
    return np.array([most] + given)


def uneven(rng, amount, total, limit, skew):
    if amount == 2:
        one = jax.random.randint(rng, (), max(1, total - limit), min(limit, total - 1) + 1)
        return jnp.stack([one, total - one])
    lengths = jnp.asarray(length_profile(amount, total, limit, skew), jnp.int32)
    couples = (amount - 1) // 2
    donor, taker = lengths[1:1 + 2 * couples:2], lengths[2:2 + 2 * couples:2]
    room = jnp.minimum(donor - 1, limit - taker)
    moved = jax.random.randint(jax.random.fold_in(rng, 1), (couples,), 0, 1 << 20) % (room + 1)
    lengths = lengths.at[1:1 + 2 * couples:2].set(donor - moved).at[2:2 + 2 * couples:2].set(taker + moved)
    return lengths[jax.random.permutation(jax.random.fold_in(rng, 2), amount)]


def scatter_about(key, extent, deviation, limit, shards=(), kind=jnp.bfloat16):
    gain = shard_levels(key, extent, shards, -0.22, 0.18) if shards else 1.0
    values = jax.random.normal(key, extent, jnp.float32) * deviation * gain
    return jnp.minimum(jnp.maximum(values, -limit), limit).astype(kind)


def setup_inputs(seed: int = 0) -> dict:
    arg_keys = jax.random.split(jax.random.key(seed), 5)
    return {
        "queries": draw_queries(jax.random.fold_in(arg_keys[4], 71), 0),
        "keys": draw_keys(jax.random.fold_in(arg_keys[4], 71), 0),
        "values": scatter_about(arg_keys[2], (PACK_TOKENS, KEY_VALUE_HEADS, HEAD_SIZE), 1.0, 6.0, ((0, 8), (1, 4))),
        "segment_ids": jnp.searchsorted(jnp.cumsum(uneven(arg_keys[3], DOCS, PACK_TOKENS, MOST, 2)), jnp.arange(PACK_TOKENS), side="right").astype(jnp.int32),
    }


def reference(queries, keys, values, segment_ids):
    tokens, heads, head = queries.shape
    groups = keys.shape[1]
    per_group = heads // groups
    block = math.gcd(tokens, 512)
    positions = jnp.arange(tokens, dtype=jnp.int32)
    scale = 1.0 / math.sqrt(head)

    def one_block(index):
        first = (index * block).astype(jnp.int32)
        query_rows = lax.dynamic_slice_in_dim(queries, first, block, 0).reshape(block, groups, per_group, head)
        seg_rows = lax.dynamic_slice_in_dim(segment_ids, first, block, 0)
        pos_rows = first + jnp.arange(block, dtype=jnp.int32)
        allowed = (seg_rows[:, None] == segment_ids[None, :]) & (positions[None, :] <= pos_rows[:, None])

        def one_group(group):
            query_group = lax.dynamic_index_in_dim(query_rows, group, 1, keepdims=False).astype(jnp.float32)
            key_group = lax.dynamic_index_in_dim(keys, group, 1, keepdims=False).astype(jnp.float32)
            value_group = lax.dynamic_index_in_dim(values, group, 1, keepdims=False).astype(jnp.float32)
            scores = jnp.einsum('tgd,pd->gtp', query_group, key_group) * scale
            scores = jnp.where(allowed[None], scores, -1e+30)
            top = lax.optimization_barrier(jnp.max(scores, axis=-1))
            weights = jnp.where(allowed[None], jnp.exp(scores - top[..., None]), 0.0)
            total = lax.optimization_barrier(jnp.sum(weights, axis=-1))
            rounded = lax.optimization_barrier(weights.astype(jnp.bfloat16)).astype(jnp.float32)
            mixed = jnp.einsum('gtp,pd->gtd', rounded, value_group)
            return mixed / total[..., None]
        result = lax.map(one_group, jnp.arange(groups, dtype=jnp.int32))
        return jnp.transpose(result, (2, 0, 1, 3)).reshape(block, heads * head).astype(jnp.bfloat16)
    output = lax.map(one_block, jnp.arange(tokens // block, dtype=jnp.int32))
    return output.reshape(tokens, heads * head)
```

```python
import functools
import math

import jax
import jax.numpy as jnp
from jax import lax
from jax.experimental import pallas as pl
from jax.experimental.pallas import tpu as pltpu
from jax.sharding import PartitionSpec as P

MESH = pl.DeviceIdType.MESH
NEG = -1e30


def plane_width(mesh):
    n = mesh.shape["ctx"]
    try:
        width = len({d.coords[1] for d in mesh.devices.flat})
    except Exception:
        width = 2
    return width if n % width == 0 else 1


def kernel(cfg, q_in, k_in, v_in, seg_ref, out_ref,
           q_ref, buf, segs, segcol, bias, acc, top, o_buf,
           kv_send, kv_recv, seg_send, seg_recv, o_send, o_recv, o_local):
    n, ny, reach, tp, groups, per_group, rows, head = cfg
    nz = n // ny
    depth = min(nz - 1, (reach + ny - 1) // ny) + 1
    out_rows = rows // tp
    const = math.log2(math.e) / math.sqrt(head)
    me = lax.axis_index("ctx")
    mt = lax.axis_index("tp")
    z = me // ny
    y = me % ny

    barrier = pltpu.get_barrier_semaphore()
    for d in range(1, reach + 1):
        @pl.when(me + d < n)
        def _():
            pl.semaphore_signal(barrier, inc=1, device_id={"ctx": me + d, "tp": mt}, device_id_type=MESH)

        @pl.when(me - d >= 0)
        def _():
            pl.semaphore_signal(barrier, inc=1, device_id={"ctx": me - d, "tp": mt}, device_id_type=MESH)
    for e in range(1, tp):
        pl.semaphore_signal(barrier, inc=1, device_id={"ctx": me, "tp": (mt + e) % tp}, device_id_type=MESH)
    peers = (tp - 1) + jnp.minimum(n - 1 - me, reach) + jnp.minimum(me, reach)
    pl.semaphore_wait(barrier, peers)

    def piece(s, dy, g, w):
        if s == 0 and dy == 0:
            return (k_in, v_in)[w].at[g]
        return buf.at[s * ny + dy, g, w]

    def sem_index(s, dy, g, w):
        return ((s * ny + dy) * groups + g) * 2 + w

    def send_index(s, e, g, w):
        return ((s * ny + e) * groups + g) * 2 + w

    def z_copy(s, g, w):
        return pltpu.make_async_remote_copy(
            src_ref=piece(s, 0, g, w),
            dst_ref=buf.at[(s + 1) * ny, g, w],
            send_sem=kv_send.at[send_index(s, 0, g, w)],
            recv_sem=kv_recv.at[sem_index(s + 1, 0, g, w)],
            device_id={"ctx": me + ny, "tp": mt},
            device_id_type=MESH,
        )

    def y_copy(s, e, g, w):
        return pltpu.make_async_remote_copy(
            src_ref=piece(s, 0, g, w),
            dst_ref=buf.at[s * ny + ny - e, g, w],
            send_sem=kv_send.at[send_index(s, e, g, w)],
            recv_sem=kv_recv.at[sem_index(s, ny - e, g, w)],
            device_id={"ctx": z * ny + (y + e) % ny, "tp": mt},
            device_id_type=MESH,
        )

    last = depth - 1
    straight = last >= 2 and last * ny > reach

    def far_copy(dy, g, w):
        return pltpu.make_async_remote_copy(
            src_ref=piece(last - 1, dy, g, w),
            dst_ref=buf.at[last * ny + dy, g, w],
            send_sem=kv_send.at[send_index(last, dy, g, w)],
            recv_sem=kv_recv.at[sem_index(last, dy, g, w)],
            device_id={"ctx": me + ny, "tp": mt},
            device_id_type=MESH,
        )

    def sends_far(dy):
        gap = me + ny - owner(last - 1, dy)
        return (z >= last - 1) & (z + 1 < nz) & (gap <= reach)

    def owner(s, dy):
        return (z - s) * ny + (y + dy) % ny

    def has_column(s):
        return (z >= s) & (s * ny <= reach)

    def sends_z(s):
        return (z >= s) & (z + 1 < nz) & ((s + 1) * ny <= reach)

    def sends_y(s, e):
        gap = z * ny + (y + e) % ny - owner(s, 0)
        return (z >= s) & (s * ny <= reach) & (gap > 0) & (gap <= reach)

    def wanted(s, dy):
        gap = me - owner(s, dy)
        return (z >= s) & (gap > 0) & (gap <= reach)

    def arrived(s, dy, g, w):
        pltpu.make_async_copy(buf.at[s * ny + dy, g, w], buf.at[s * ny + dy, g, w],
                              kv_recv.at[sem_index(s, dy, g, w)]).wait()

    def push(s, g):
        for w in range(2):
            if s > 0:
                @pl.when(has_column(s))
                def _():
                    arrived(s, 0, g, w)
            if s + 1 < depth:
                @pl.when(sends_z(s))
                def _():
                    z_copy(s, g, w).start()
            for e in range(1, ny):
                @pl.when(sends_y(s, e))
                def _():
                    y_copy(s, e, g, w).start()

    def seg_copy(d):
        return pltpu.make_async_remote_copy(
            src_ref=seg_ref,
            dst_ref=segs.at[d],
            send_sem=seg_send.at[d],
            recv_sem=seg_recv.at[d],
            device_id={"ctx": me + d, "tp": mt},
            device_id_type=MESH,
        )

    push(0, 0)
    for d in range(1, reach + 1):
        @pl.when(me + d < n)
        def _():
            seg_copy(d).start()

    for i in range(groups * per_group):
        q_ref[i] = q_in[:, i, :]
    segcol[...] = jnp.transpose(jnp.broadcast_to(seg_ref[...], (head, rows)))

    def attend(s, dy, g, first):
        k_ref, v_ref = piece(s, dy, g, 0), piece(s, dy, g, 1)
        if first:
            seg_k = seg_ref[...]
        else:
            seg_k = segs[me - owner(s, dy)]
        column = segcol[...]
        allowed = jnp.concatenate([column] * (rows // head), axis=1) == seg_k
        if first:
            r = lax.broadcasted_iota(jnp.int32, (rows, rows), 0)
            c = lax.broadcasted_iota(jnp.int32, (rows, rows), 1)
            allowed = allowed & (c <= r)
        bias[...] = jnp.where(allowed, 0.0, NEG)

        def one(h, carry):
            i = g * per_group + h
            scores = lax.dot_general(q_ref[i], k_ref[...], (((1,), (1,)), ((), ())),
                                     preferred_element_type=jnp.float32)
            scores = scores * const + bias[...]
            high = jnp.broadcast_to(jnp.max(scores, axis=1, keepdims=True), (rows, head))
            if not first:
                old = top[i]
                high = jnp.maximum(old, high)
            weights = jnp.exp2(scores - jnp.concatenate([high] * (rows // head), axis=1)).astype(jnp.bfloat16)
            v = jnp.concatenate([v_ref[...], jnp.ones((rows, head), jnp.bfloat16)], axis=1)
            mixed = jnp.dot(weights, v, preferred_element_type=jnp.float32)
            if not first:
                factor = jnp.exp2(old - high)
                mixed = acc[i] * jnp.concatenate([factor, factor], axis=1) + mixed
            acc[i] = mixed
            top[i] = high
            return carry

        lax.fori_loop(0, per_group, one, 0, unroll=per_group)

    def attend_y(s, g):
        for dy in range(1, ny):
            @pl.when(wanted(s, dy))
            def _():
                arrived(s, dy, g, 0)
                arrived(s, dy, g, 1)
                if straight and s == last - 1:
                    @pl.when(sends_far(dy))
                    def _():
                        far_copy(dy, g, 0).start()
                        far_copy(dy, g, 1).start()
                attend(s, dy, g, False)

    per_send = max(per_group // 2, 1)
    width = per_send * head
    pieces = per_group // per_send

    def o_copy(c, e):
        col = pl.multiple_of((mt * groups * pieces + c) * width, width)
        to = (mt + e) % tp
        return pltpu.make_async_remote_copy(
            src_ref=o_buf.at[pl.ds(pl.multiple_of(to * out_rows, out_rows), out_rows), pl.ds(c * width, width)],
            dst_ref=out_ref.at[:, pl.ds(col, width)],
            send_sem=o_send.at[c * tp + e],
            recv_sem=o_recv.at[c * tp + e],
            device_id={"ctx": me, "tp": to},
            device_id_type=MESH,
        )

    def o_own(c):
        col = pl.multiple_of((mt * groups * pieces + c) * width, width)
        return pltpu.make_async_copy(
            o_buf.at[pl.ds(pl.multiple_of(mt * out_rows, out_rows), out_rows), pl.ds(c * width, width)],
            out_ref.at[:, pl.ds(col, width)],
            o_local.at[c],
        )

    def finish(g):
        for p in range(pieces):
            c = g * pieces + p
            for h in range(per_send):
                i = g * per_group + p * per_send + h
                o_buf[:, i * head:(i + 1) * head] = (acc[i, :, :head] / acc[i, :, head:]).astype(jnp.bfloat16)
            for e in range(1, tp):
                o_copy(c, e).start()
            o_own(c).start()

    for g in range(groups):
        attend(0, 0, g, True)
        if g == 0:
            for d in range(1, reach + 1):
                @pl.when(me - d >= 0)
                def _():
                    pltpu.make_async_copy(segs.at[d], segs.at[d], seg_recv.at[d]).wait()
        for s in range(1, depth):
            push(s, g)
            if s == depth - 1 and g + 1 < groups:
                push(0, g + 1)

            @pl.when(wanted(s, 0))
            def _():
                attend(s, 0, g, False)
            attend_y(s - 1, g)
        if depth == 1 and g + 1 < groups:
            push(0, g + 1)
        attend_y(depth - 1, g)
        finish(g)

    for s in range(depth):
        for g in range(groups):
            for w in range(2):
                if s + 1 < depth:
                    @pl.when(sends_z(s))
                    def _():
                        z_copy(s, g, w).wait_send()
                for e in range(1, ny):
                    @pl.when(sends_y(s, e))
                    def _():
                        y_copy(s, e, g, w).wait_send()
    if straight:
        for g in range(groups):
            for w in range(2):
                for dy in range(1, ny):
                    @pl.when(wanted(last - 1, dy) & sends_far(dy))
                    def _():
                        far_copy(dy, g, w).wait_send()
    for d in range(1, reach + 1):
        @pl.when(me + d < n)
        def _():
            seg_copy(d).wait_send()
    for c in range(groups * pieces):
        o_own(c).wait()
        for e in range(1, tp):
            o_copy(c, e).wait()


def local(ny, queries, keys, values, segment_ids):
    rows, heads, head = queries.shape
    groups = keys.shape[1]
    per_group = heads // groups
    n = lax.axis_size("ctx")
    tp = lax.axis_size("tp")
    nz = n // ny
    longest = rows * n * 5 // 8
    reach = min((longest + rows - 1) // rows, n - 1)
    depth = min(nz - 1, (reach + ny - 1) // ny) + 1
    k = jnp.transpose(keys, (1, 0, 2))
    v = jnp.transpose(values, (1, 0, 2))
    pieces = groups * (per_group // max(per_group // 2, 1))
    slots = depth * ny
    vmem = pl.BlockSpec(memory_space=pltpu.VMEM)
    dma = pltpu.SemaphoreType.DMA
    cfg = (n, ny, reach, tp, groups, per_group, rows, head)
    return pl.pallas_call(
        functools.partial(kernel, cfg),
        out_shape=pltpu.VMEM((rows // tp, tp * heads * head), jnp.bfloat16),
        in_specs=[vmem] * 4,
        out_specs=vmem,
        scratch_shapes=[
            pltpu.VMEM((heads, rows, head), jnp.bfloat16),
            pltpu.VMEM((slots, groups, 2, rows, head), jnp.bfloat16),
            pltpu.VMEM((reach + 1, 1, rows), jnp.int32),
            pltpu.VMEM((rows, head), jnp.int32),
            pltpu.VMEM((rows, rows), jnp.float32),
            pltpu.VMEM((heads, rows, 2 * head), jnp.float32),
            pltpu.VMEM((heads, rows, head), jnp.float32),
            pltpu.VMEM((rows, heads * head), jnp.bfloat16),
            dma((slots * groups * 2,)),
            dma((slots * groups * 2,)),
            dma((reach + 1,)),
            dma((reach + 1,)),
            dma((pieces * tp,)),
            dma((pieces * tp,)),
            dma((pieces,)),
        ],
        compiler_params=pltpu.CompilerParams(
            collective_id=0, has_side_effects=True, vmem_limit_bytes=56 * 1024 * 1024
        ),
    )(queries, k, v, segment_ids.reshape(1, rows))


def solution(mesh):
    in_specs = (P("ctx", "tp", None), P("ctx", "tp", None), P("ctx", "tp", None), P("ctx"))
    out_specs = P(("ctx", "tp"), None)
    body = functools.partial(local, plane_width(mesh))
    return jax.shard_map(body, mesh=mesh, in_specs=in_specs, out_specs=out_specs, check_vma=False)
```

```python
import functools
import math

import jax
import jax.numpy as jnp
from jax import lax
from jax.experimental import pallas as pl
from jax.experimental.pallas import tpu as pltpu
from jax.sharding import PartitionSpec as P

MESH = pl.DeviceIdType.MESH
NEG = -1e30


def plane_width(mesh):
    n = mesh.shape["ctx"]
    try:
        width = len({d.coords[1] for d in mesh.devices.flat})
    except Exception:
        width = 2
    return width if n % width == 0 else 1


def kernel(cfg, q_in, k_in, v_in, seg_ref, out_ref,
           q_ref, buf, segs, segcol, bias, acc, top, o_buf,
           kv_send, kv_recv, seg_send, seg_recv, o_send, o_recv, o_local):
    n, ny, reach, tp, groups, per_group, rows, head = cfg
    nz = n // ny
    depth = min(nz - 1, (reach + ny - 1) // ny) + 1
    out_rows = rows // tp
    const = math.log2(math.e) / math.sqrt(head)
    me = lax.axis_index("ctx")
    mt = lax.axis_index("tp")
    z = me // ny
    y = me % ny

    barrier = pltpu.get_barrier_semaphore()
    for d in range(1, reach + 1):
        @pl.when(me + d < n)
        def _():
            pl.semaphore_signal(barrier, inc=1, device_id={"ctx": me + d, "tp": mt}, device_id_type=MESH)

        @pl.when(me - d >= 0)
        def _():
            pl.semaphore_signal(barrier, inc=1, device_id={"ctx": me - d, "tp": mt}, device_id_type=MESH)
    for e in range(1, tp):
        pl.semaphore_signal(barrier, inc=1, device_id={"ctx": me, "tp": (mt + e) % tp}, device_id_type=MESH)
    peers = (tp - 1) + jnp.minimum(n - 1 - me, reach) + jnp.minimum(me, reach)
    pl.semaphore_wait(barrier, peers)

    def piece(s, dy, g, w):
        if s == 0 and dy == 0:
            return (k_in, v_in)[w].at[g]
        return buf.at[s * ny + dy, g, w]

    def sem_index(s, dy, g, w):
        return ((s * ny + dy) * groups + g) * 2 + w

    def send_index(s, e, g, w):
        return ((s * ny + e) * groups + g) * 2 + w

    def z_copy(s, g, w):
        return pltpu.make_async_remote_copy(
            src_ref=piece(s, 0, g, w),
            dst_ref=buf.at[(s + 1) * ny, g, w],
            send_sem=kv_send.at[send_index(s, 0, g, w)],
            recv_sem=kv_recv.at[sem_index(s + 1, 0, g, w)],
            device_id={"ctx": me + ny, "tp": mt},
            device_id_type=MESH,
        )

    def y_copy(s, e, g, w):
        return pltpu.make_async_remote_copy(
            src_ref=piece(s, 0, g, w),
            dst_ref=buf.at[s * ny + ny - e, g, w],
            send_sem=kv_send.at[send_index(s, e, g, w)],
            recv_sem=kv_recv.at[sem_index(s, ny - e, g, w)],
            device_id={"ctx": z * ny + (y + e) % ny, "tp": mt},
            device_id_type=MESH,
        )

    last = depth - 1
    straight = last >= 2 and last * ny > reach

    def far_copy(dy, g, w):
        return pltpu.make_async_remote_copy(
            src_ref=piece(last - 1, dy, g, w),
            dst_ref=buf.at[last * ny + dy, g, w],
            send_sem=kv_send.at[send_index(last, dy, g, w)],
            recv_sem=kv_recv.at[sem_index(last, dy, g, w)],
            device_id={"ctx": me + ny, "tp": mt},
            device_id_type=MESH,
        )

    def sends_far(dy):
        gap = me + ny - owner(last - 1, dy)
        return (z >= last - 1) & (z + 1 < nz) & (gap <= reach)

    def owner(s, dy):
        return (z - s) * ny + (y + dy) % ny

    def has_column(s):
        return (z >= s) & (s * ny <= reach)

    def sends_z(s):
        return (z >= s) & (z + 1 < nz) & ((s + 1) * ny <= reach)

    def sends_y(s, e):
        gap = z * ny + (y + e) % ny - owner(s, 0)
        return (z >= s) & (s * ny <= reach) & (gap > 0) & (gap <= reach)

    def wanted(s, dy):
        gap = me - owner(s, dy)
        return (z >= s) & (gap > 0) & (gap <= reach)

    def arrived(s, dy, g, w):
        pltpu.make_async_copy(buf.at[s * ny + dy, g, w], buf.at[s * ny + dy, g, w],
                              kv_recv.at[sem_index(s, dy, g, w)]).wait()

    def push(s, g):
        for w in range(2):
            if s > 0:
                @pl.when(has_column(s))
                def _():
                    arrived(s, 0, g, w)
            if s + 1 < depth:
                @pl.when(sends_z(s))
                def _():
                    z_copy(s, g, w).start()
            for e in range(1, ny):
                @pl.when(sends_y(s, e))
                def _():
                    y_copy(s, e, g, w).start()

    def seg_copy(d):
        return pltpu.make_async_remote_copy(
            src_ref=seg_ref,
            dst_ref=segs.at[d],
            send_sem=seg_send.at[d],
            recv_sem=seg_recv.at[d],
            device_id={"ctx": me + d, "tp": mt},
            device_id_type=MESH,
        )

    push(0, 0)
    for d in range(1, reach + 1):
        @pl.when(me + d < n)
        def _():
            seg_copy(d).start()

    for i in range(groups * per_group):
        q_ref[i] = q_in[:, i, :]
    segcol[...] = jnp.transpose(jnp.broadcast_to(seg_ref[...], (head, rows)))

    def attend(s, dy, g, first):
        k_ref, v_ref = piece(s, dy, g, 0), piece(s, dy, g, 1)
        if first:
            seg_k = seg_ref[...]
        else:
            seg_k = segs[me - owner(s, dy)]
        column = segcol[...]
        allowed = jnp.concatenate([column] * (rows // head), axis=1) == seg_k
        if first:
            r = lax.broadcasted_iota(jnp.int32, (rows, rows), 0)
            c = lax.broadcasted_iota(jnp.int32, (rows, rows), 1)
            allowed = allowed & (c <= r)
        bias[...] = jnp.where(allowed, 0.0, NEG)

        def one(h, carry):
            i = g * per_group + h
            scores = lax.dot_general(q_ref[i], k_ref[...], (((1,), (1,)), ((), ())),
                                     preferred_element_type=jnp.float32)
            scores = scores * const + bias[...]
            high = jnp.broadcast_to(jnp.max(scores, axis=1, keepdims=True), (rows, head))
            if not first:
                old = top[i]
                high = jnp.maximum(old, high)
            weights = jnp.exp2(scores - jnp.concatenate([high] * (rows // head), axis=1)).astype(jnp.bfloat16)
            v = jnp.concatenate([v_ref[...], jnp.ones((rows, head), jnp.bfloat16)], axis=1)
            mixed = jnp.dot(weights, v, preferred_element_type=jnp.float32)
            if not first:
                factor = jnp.exp2(old - high)
                mixed = acc[i] * jnp.concatenate([factor, factor], axis=1) + mixed
            acc[i] = mixed
            top[i] = high
            return carry

        lax.fori_loop(0, per_group, one, 0, unroll=per_group)

    def attend_y(s, g):
        for dy in range(1, ny):
            @pl.when(wanted(s, dy))
            def _():
                arrived(s, dy, g, 0)
                arrived(s, dy, g, 1)
                if straight and s == last - 1:
                    @pl.when(sends_far(dy))
                    def _():
                        far_copy(dy, g, 0).start()
                        far_copy(dy, g, 1).start()
                attend(s, dy, g, False)

    per_send = max(per_group // 2, 1)
    width = per_send * head
    pieces = per_group // per_send

    def o_copy(c, e):
        col = pl.multiple_of((mt * groups * pieces + c) * width, width)
        to = (mt + e) % tp
        return pltpu.make_async_remote_copy(
            src_ref=o_buf.at[pl.ds(pl.multiple_of(to * out_rows, out_rows), out_rows), pl.ds(c * width, width)],
            dst_ref=out_ref.at[:, pl.ds(col, width)],
            send_sem=o_send.at[c * tp + e],
            recv_sem=o_recv.at[c * tp + e],
            device_id={"ctx": me, "tp": to},
            device_id_type=MESH,
        )

    def o_own(c):
        col = pl.multiple_of((mt * groups * pieces + c) * width, width)
        return pltpu.make_async_copy(
            o_buf.at[pl.ds(pl.multiple_of(mt * out_rows, out_rows), out_rows), pl.ds(c * width, width)],
            out_ref.at[:, pl.ds(col, width)],
            o_local.at[c],
        )

    def finish(g):
        for p in range(pieces):
            c = g * pieces + p
            for h in range(per_send):
                i = g * per_group + p * per_send + h
                o_buf[:, i * head:(i + 1) * head] = (acc[i, :, :head] / acc[i, :, head:]).astype(jnp.bfloat16)
            for e in range(1, tp):
                o_copy(c, e).start()
            o_own(c).start()

    for g in range(groups):
        attend(0, 0, g, True)
        if g == 0:
            for d in range(1, reach + 1):
                @pl.when(me - d >= 0)
                def _():
                    pltpu.make_async_copy(segs.at[d], segs.at[d], seg_recv.at[d]).wait()
        for s in range(1, depth):
            push(s, g)
            if s == depth - 1 and g + 1 < groups:
                push(0, g + 1)

            @pl.when(wanted(s, 0))
            def _():
                attend(s, 0, g, False)
            attend_y(s - 1, g)
        if depth == 1 and g + 1 < groups:
            push(0, g + 1)
        attend_y(depth - 1, g)
        finish(g)

    for s in range(depth):
        for g in range(groups):
            for w in range(2):
                if s + 1 < depth:
                    @pl.when(sends_z(s))
                    def _():
                        z_copy(s, g, w).wait_send()
                for e in range(1, ny):
                    @pl.when(sends_y(s, e))
                    def _():
                        y_copy(s, e, g, w).wait_send()
    if straight:
        for g in range(groups):
            for w in range(2):
                for dy in range(1, ny):
                    @pl.when(wanted(last - 1, dy) & sends_far(dy))
                    def _():
                        far_copy(dy, g, w).wait_send()
    for d in range(1, reach + 1):
        @pl.when(me + d < n)
        def _():
            seg_copy(d).wait_send()
    for c in range(groups * pieces):
        o_own(c).wait()
        for e in range(1, tp):
            o_copy(c, e).wait()


def local(ny, queries, keys, values, segment_ids):
    rows, heads, head = queries.shape
    groups = keys.shape[1]
    per_group = heads // groups
    n = lax.axis_size("ctx")
    tp = lax.axis_size("tp")
    nz = n // ny
    longest = rows * n * 5 // 8
    reach = min((longest + rows - 1) // rows, n - 1)
    depth = min(nz - 1, (reach + ny - 1) // ny) + 1
    k = jnp.transpose(keys, (1, 0, 2))
    v = jnp.transpose(values, (1, 0, 2))
    pieces = groups * (per_group // max(per_group // 2, 1))
    slots = depth * ny
    vmem = pl.BlockSpec(memory_space=pltpu.VMEM)
    dma = pltpu.SemaphoreType.DMA
    cfg = (n, ny, reach, tp, groups, per_group, rows, head)
    return pl.pallas_call(
        functools.partial(kernel, cfg),
        out_shape=pltpu.VMEM((rows // tp, tp * heads * head), jnp.bfloat16),
        in_specs=[vmem] * 4,
        out_specs=vmem,
        scratch_shapes=[
            pltpu.VMEM((heads, rows, head), jnp.bfloat16),
            pltpu.VMEM((slots, groups, 2, rows, head), jnp.bfloat16),
            pltpu.VMEM((reach + 1, 1, rows), jnp.int32),
            pltpu.VMEM((rows, head), jnp.int32),
            pltpu.VMEM((rows, rows), jnp.float32),
            pltpu.VMEM((heads, rows, 2 * head), jnp.float32),
            pltpu.VMEM((heads, rows, head), jnp.float32),
            pltpu.VMEM((rows, heads * head), jnp.bfloat16),
            dma((slots * groups * 2,)),
            dma((slots * groups * 2,)),
            dma((reach + 1,)),
            dma((reach + 1,)),
            dma((pieces * tp,)),
            dma((pieces * tp,)),
            dma((pieces,)),
        ],
        compiler_params=pltpu.CompilerParams(
            collective_id=0, has_side_effects=True, vmem_limit_bytes=56 * 1024 * 1024
        ),
    )(queries, k, v, segment_ids.reshape(1, rows))


UNITS = (
    (0, 0, 0, 0, 0, 0, 0, 0),
    (0, 0, 0, 0, 0, 0, 0, 0),
    (0, 0, 16, 16, 18, 19, 20, 21),
    (0, 0, 0, 18, 19, 27, 21, 22),
    (0, 0, 0, 0, 16, 20, 18, 19),
    (0, 0, 0, 0, 0, 28, 28, 20),
    (0, 0, 0, 0, 0, 18, 19, 0),
    (0, 0, 0, 0, 0, 16, 0, 0),
    (0, 16, 17, 17, 17, 17, 17, 18),
    (0, 0, 24, 26, 27, 26, 26, 28),
    (0, 0, 0, 24, 26, 24, 29, 29),
    (0, 0, 0, 0, 25, 0, 25, 27),
    (0, 0, 0, 0, 0, 0, 0, 30),
    (0, 24, 25, 25, 24, 25, 27, 26),
)
EVENTS = (
    (
        (2152, 2209, 2170, 2091, 2172, 2101, 2118, 0),
        (2144, 2217, 2154, 2083, 0, 2085, 0, 0),
        (0, 0, 2146, 2099, 0, 2093, 0, 0),
        (0, 0, 2144, 0, 0, 0, 0, 0),
        (0, 0, 2152, 0, 0, 0, 0, 0),
    ),
    (
        (0, 0, 0, 2107, 2148, 2147, 2140, 0),
        (0, 0, 0, 0, 2164, 0, 2116, 0),
        (0, 0, 0, 0, 2156, 0, 0, 0),
    ),
    (
        (2160, 2233, 2081, 2089, 0, 2155, 2126, 2133),
        (0, 0, 2136, 0, 0, 0, 0, 0),
    ),
    (
        (0, 0, 0, 2058, 2154, 2109, 0, 2054),
        (0, 0, 0, 2050, 2112, 2163, 0, 2117),
        (0, 0, 0, 2048, 2146, 0, 0, 0),
        (0, 0, 0, 2074, 0, 0, 0, 0),
        (0, 0, 0, 2105, 0, 0, 0, 0),
        (0, 0, 0, 2088, 0, 0, 0, 0),
    ),
    (
        (2168, 2056, 0, 0, 2170, 2060, 2124, 2125),
        (0, 0, 0, 0, 0, 2052, 2058, 2052),
        (0, 0, 0, 0, 0, 2171, 0, 2115),
    ),
    (
        (0, 2225, 2089, 2104, 2056, 0, 2053, 2076),
        (0, 0, 0, 0, 2059, 0, 2069, 0),
        (0, 0, 0, 0, 2051, 0, 0, 0),
    ),
    (
        (0, 2048, 2162, 0, 2145, 0, 2132, 2062),
        (0, 0, 0, 0, 0, 0, 2114, 2123),
        (0, 0, 0, 0, 0, 0, 2061, 0),
    ),
    (
        (0, 0, 0, 0, 0, 0, 0, 2060),
        (0, 0, 0, 0, 0, 0, 0, 2141),
    ),
    (
        (0, 0, 0, 2065, 0, 2076, 0, 0),
    ),
    (
        (0, 0, 0, 2049, 2089, 0, 2134, 0),
        (0, 0, 0, 0, 2067, 0, 0, 0),
        (0, 0, 0, 0, 2162, 0, 0, 0),
    ),
    (
        (0, 0, 0, 0, 0, 2090, 0, 2139),
        (0, 0, 0, 0, 0, 2137, 0, 0),
        (0, 0, 0, 0, 0, 2068, 0, 0),
        (0, 0, 0, 0, 0, 2048, 0, 0),
    ),
    (
        (0, 0, 0, 0, 0, 0, 0, 2131),
        (0, 0, 0, 0, 0, 0, 0, 2050),
        (0, 0, 0, 0, 0, 0, 0, 2068),
    ),
    (
        (0, 0, 0, 0, 0, 2050, 2051, 2058),
        (0, 0, 0, 0, 0, 2056, 2142, 0),
        (0, 0, 0, 0, 0, 0, 2059, 0),
    ),
    (),
    (
        (0, 0, 0, 0, 0, 0, 2057, 0),
    ),
    (
        (0, 0, 0, 0, 0, 0, 2049, 0),
    ),
    (
        (0, 0, 0, 0, 0, 2057, 0, 0),
        (0, 0, 0, 0, 0, 2074, 0, 0),
        (0, 0, 0, 0, 0, 2136, 0, 0),
        (0, 0, 0, 0, 0, 2049, 0, 0),
    ),
    (
        (0, 0, 2160, 0, 2075, 2064, 2138, 0),
    ),
    (
        (0, 2072, 0, 2066, 2128, 2066, 2130, 0),
        (0, 0, 0, 2064, 2105, 0, 2077, 0),
    ),
    (
        (0, 2064, 0, 0, 0, 0, 0, 0),
    ),
    (
        (0, 0, 2097, 0, 2161, 0, 2075, 0),
        (0, 0, 0, 0, 0, 0, 2073, 0),
    ),
    (
        (0, 0, 2073, 0, 0, 0, 0, 0),
    ),
    (
        (0, 0, 0, 0, 0, 2065, 2067, 0),
        (0, 0, 0, 0, 0, 0, 2065, 0),
    ),
    (
        (0, 0, 0, 0, 2072, 0, 0, 2070),
    ),
    (
        (0, 0, 0, 0, 0, 0, 0, 2078),
        (0, 0, 0, 0, 0, 0, 0, 2074),
    ),
    (
        (0, 0, 0, 0, 0, 0, 0, 2066),
    ),
    (),
    (),
    (),
)
LAST = (8, 13)


def targets(code, me):
    found = []
    if code // 2048 % 2:
        if code // 32 % 2:
            found.append(me + 2)
        if code // 64 % 2:
            found.append(me ^ 1)
        if code // 128 % 8:
            found.append(me + code // 128 % 8)
    return found


def planned_kernel(cfg, q_hbm, k_hbm, v_hbm, seg_hbm, out_ref,
                   q_raw, kv_raw, q_ref, buf, segs, segcol, bias, acc, top, o_buf,
                   load, kv_send, kv_recv, seg_send, seg_recv, o_send, o_recv):
    n, tp, groups, per_group, rows, head = cfg
    out_rows = rows // tp
    const = math.log2(math.e) / math.sqrt(head)
    me = lax.axis_index("ctx")
    mt = lax.axis_index("tp")

    def pick(values):
        usual = max(set(values), key=values.count)
        chosen = jnp.int32(usual)
        for d, value in enumerate(values):
            if value != usual:
                chosen = jnp.where(me == d, jnp.int32(value), chosen)
        return chosen

    k_load = pltpu.make_async_copy(k_hbm, kv_raw.at[0], load.at[0])
    v_load = pltpu.make_async_copy(v_hbm, kv_raw.at[1], load.at[1])
    seg_load = pltpu.make_async_copy(seg_hbm, segs.at[me], load.at[2])
    q_load = pltpu.make_async_copy(q_hbm, q_raw, load.at[3])
    k_load.start()
    v_load.start()
    seg_load.start()
    q_load.start()

    edges = sorted({(m, t) for step in EVENTS for slot in step for m, code in enumerate(slot) for t in targets(code, m)})
    barrier = pltpu.get_barrier_semaphore()
    for s, d in edges:
        @pl.when(me == d)
        def _():
            pl.semaphore_signal(barrier, inc=1, device_id={"ctx": s, "tp": mt}, device_id_type=MESH)
    for e in range(1, tp):
        pl.semaphore_signal(barrier, inc=1, device_id={"ctx": me, "tp": (mt + e) % tp}, device_id_type=MESH)
    k_load.wait()
    v_load.wait()
    for w in range(2):
        for g in range(groups):
            buf[me, g, w] = kv_raw[w, :, g, :]
    seg_load.wait()
    pl.semaphore_wait(barrier, pick([sum(s == m for s, _ in edges) for m in range(n)]) + (tp - 1))

    def piece_copy(b, gw, way, to):
        index = b * (2 * groups) + gw
        return pltpu.make_async_remote_copy(
            src_ref=buf.at[b, gw // 2, gw % 2],
            dst_ref=buf.at[b, gw // 2, gw % 2],
            send_sem=kv_send.at[index * 3 + way],
            recv_sem=kv_recv.at[index],
            device_id={"ctx": to, "tp": mt},
            device_id_type=MESH,
        )

    def seg_copy(b, way, to):
        return pltpu.make_async_remote_copy(
            src_ref=segs.at[b],
            dst_ref=segs.at[b],
            send_sem=seg_send.at[b * 3 + way],
            recv_sem=seg_recv.at[b],
            device_id={"ctx": to, "tp": mt},
            device_id_type=MESH,
        )

    def routes(slot):
        code = pick(slot)
        b, gw, far = code % 8, code // 8 % 4, code // 128 % 8
        ways = []
        if any(v // 32 % 2 for v in slot):
            ways.append((0, code // 32 % 2 == 1, me + 2))
        if any(v // 64 % 2 for v in slot):
            ways.append((1, code // 64 % 2 == 1, me + 1 - 2 * (me % 2)))
        if any(v // 128 % 8 for v in slot):
            ways.append((2, far > 0, me + far))
        return code, b, gw, ways

    def event(slot):
        code, b, gw, ways = routes(slot)
        head_piece = any(v // 2048 and v // 8 % 4 == 0 for v in slot)

        @pl.when(code // 2048 == 1)
        def _():
            @pl.when(b != me)
            def _():
                pltpu.make_async_copy(buf.at[b, gw // 2, gw % 2], buf.at[b, gw // 2, gw % 2],
                                      kv_recv.at[b * (2 * groups) + gw]).wait()
            for way, on, to in ways:
                @pl.when(on)
                def _():
                    piece_copy(b, gw, way, to).start()
            if head_piece:
                @pl.when(gw == 0)
                def _():
                    @pl.when(b != me)
                    def _():
                        pltpu.make_async_copy(segs.at[b], segs.at[b], seg_recv.at[b]).wait()
                    for way, on, to in ways:
                        @pl.when(on)
                        def _():
                            seg_copy(b, way, to).start()

    def drain(slot):
        code, b, gw, ways = routes(slot)
        head_piece = any(v // 2048 and v // 8 % 4 == 0 for v in slot)

        @pl.when(code // 2048 == 1)
        def _():
            for way, on, to in ways:
                @pl.when(on)
                def _():
                    piece_copy(b, gw, way, to).wait_send()
            if head_piece:
                @pl.when(gw == 0)
                def _():
                    for way, on, to in ways:
                        @pl.when(on)
                        def _():
                            seg_copy(b, way, to).wait_send()

    def one(g, h, k_ref, v_ref, first):
        i = g * per_group + h
        scores = lax.dot_general(q_ref[i], k_ref[...], (((1,), (1,)), ((), ())),
                                 preferred_element_type=jnp.float32)
        scores = scores * const + bias[...]
        high = jnp.broadcast_to(jnp.max(scores, axis=1, keepdims=True), (rows, head))
        if not first:
            old = top[i]
            high = jnp.maximum(old, high)
        weights = jnp.exp2(scores - jnp.concatenate([high] * (rows // head), axis=1)).astype(jnp.bfloat16)
        v = jnp.concatenate([v_ref[...], jnp.ones((rows, head), jnp.bfloat16)], axis=1)
        mixed = jnp.dot(weights, v, preferred_element_type=jnp.float32)
        if not first:
            factor = jnp.exp2(old - high)
            mixed = acc[i] * jnp.concatenate([factor, factor], axis=1) + mixed
        acc[i] = mixed
        top[i] = high

    def set_bias(b, first):
        allowed = jnp.concatenate([segcol[...]] * (rows // head), axis=1) == segs[b]
        if first:
            r = lax.broadcasted_iota(jnp.int32, (rows, rows), 0)
            c = lax.broadcasted_iota(jnp.int32, (rows, rows), 1)
            allowed = allowed & (c <= r)
        bias[...] = jnp.where(allowed, 0.0, NEG)

    def unit(values, half):
        code = pick(values)
        b, g = code % 8, code // 8 % 2

        @pl.when(code // 16 == 1)
        def _():
            if half == 0:
                set_bias(b, False)
            for h in halves[half]:
                one(g, h, buf.at[b, g, 0], buf.at[b, g, 1], False)

    halves = (range(per_group // 2), range(per_group // 2, per_group))
    per_send = 2
    width = per_send * head
    pieces = per_group // per_send

    def o_copy(c, e):
        col = pl.multiple_of((mt * groups * pieces + c) * width, width)
        to = (mt + e) % tp
        return pltpu.make_async_remote_copy(
            src_ref=o_buf.at[pl.ds(pl.multiple_of(to * out_rows, out_rows), out_rows), pl.ds(c * width, width)],
            dst_ref=out_ref.at[:, pl.ds(col, width)],
            send_sem=o_send.at[c * tp + e],
            recv_sem=o_recv.at[c * tp + e],
            device_id={"ctx": me, "tp": to},
            device_id_type=MESH,
        )

    def last_unit(values, g, half):
        code = pick(values)
        b = code % 8
        live = code // 16 == 1

        if half == 0:
            @pl.when(live)
            def _():
                set_bias(b, False)
        for p in range(half * pieces // 2, (half + 1) * pieces // 2):
            @pl.when(live)
            def _():
                for h in range(per_send):
                    one(g, p * per_send + h, buf.at[b, g, 0], buf.at[b, g, 1], False)
            c = g * pieces + p
            for h in range(per_send):
                i = g * per_group + p * per_send + h
                o_buf[:, i * head:(i + 1) * head] = (acc[i, :, :head] / acc[i, :, head:]).astype(jnp.bfloat16)
            for e in range(1, tp):
                o_copy(c, e).start()
            mine = pl.ds(pl.multiple_of(mt * out_rows, out_rows), out_rows)
            col = pl.multiple_of((mt * groups * pieces + c) * width, width)
            out_ref[:, pl.ds(col, width)] = o_buf[mine, c * width:(c + 1) * width]

    for slot in EVENTS[0]:
        event(slot)
    q_load.wait()
    segcol[...] = jnp.transpose(jnp.broadcast_to(segs[me], (head, rows)))
    set_bias(me, True)
    for step, values in enumerate(UNITS):
        for half in range(2):
            if step + half > 0:
                for slot in EVENTS[2 * step + half]:
                    event(slot)
            if step < groups:
                for h in halves[half]:
                    q_ref[step * per_group + h] = q_raw[:, step * per_group + h, :]
                for h in halves[half]:
                    one(step, h, buf.at[me, step, 0], buf.at[me, step, 1], True)
            elif step in LAST:
                last_unit(values, LAST.index(step), half)
            else:
                unit(values, half)
    for slot in EVENTS[2 * len(UNITS)]:
        event(slot)

    for group in EVENTS:
        for slot in group:
            drain(slot)
    for c in range(groups * pieces):
        for e in range(1, tp):
            o_copy(c, e).wait()


def planned(queries, keys, values, segment_ids):
    rows, heads, head = queries.shape
    groups = keys.shape[1]
    per_group = heads // groups
    n = lax.axis_size("ctx")
    tp = lax.axis_size("tp")
    chunks = groups * per_group // 2
    hbm = pl.BlockSpec(memory_space=pltpu.HBM)
    dma = pltpu.SemaphoreType.DMA
    cfg = (n, tp, groups, per_group, rows, head)
    return pl.pallas_call(
        functools.partial(planned_kernel, cfg),
        out_shape=pltpu.VMEM((rows // tp, tp * heads * head), jnp.bfloat16),
        in_specs=[hbm] * 4,
        out_specs=pl.BlockSpec(memory_space=pltpu.VMEM),
        scratch_shapes=[
            pltpu.VMEM((rows, heads, head), jnp.bfloat16),
            pltpu.VMEM((2, rows, groups, head), jnp.bfloat16),
            pltpu.VMEM((heads, rows, head), jnp.bfloat16),
            pltpu.VMEM((n, groups, 2, rows, head), jnp.bfloat16),
            pltpu.VMEM((n, 1, rows), jnp.int32),
            pltpu.VMEM((rows, head), jnp.int32),
            pltpu.VMEM((rows, rows), jnp.float32),
            pltpu.VMEM((heads, rows, 2 * head), jnp.float32),
            pltpu.VMEM((heads, rows, head), jnp.float32),
            pltpu.VMEM((rows, heads * head), jnp.bfloat16),
            dma((4,)),
            dma((n * groups * 2 * 3,)),
            dma((n * groups * 2,)),
            dma((n * 3,)),
            dma((n,)),
            dma((chunks * tp,)),
            dma((chunks * tp,)),
        ],
        compiler_params=pltpu.CompilerParams(
            collective_id=0, has_side_effects=True, vmem_limit_bytes=56 * 1024 * 1024
        ),
    )(queries, keys, values, segment_ids.reshape(1, rows))


def fits_plan(mesh):
    n = mesh.shape["ctx"]
    return plane_width(mesh) == 2 and n == len(UNITS[0])


def solution(mesh):
    in_specs = (P("ctx", "tp", None), P("ctx", "tp", None), P("ctx", "tp", None), P("ctx"))
    out_specs = P(("ctx", "tp"), None)
    body = planned if fits_plan(mesh) else functools.partial(local, plane_width(mesh))
    return jax.shard_map(body, mesh=mesh, in_specs=in_specs, out_specs=out_specs, check_vma=False)
```

```python
import functools
import math

import jax
import jax.numpy as jnp
from jax import lax
from jax.experimental import pallas as pl
from jax.experimental.pallas import tpu as pltpu
from jax.sharding import PartitionSpec as P

MESH = pl.DeviceIdType.MESH
NEG = -1e30


def plane_width(mesh):
    n = mesh.shape["ctx"]
    try:
        width = len({d.coords[1] for d in mesh.devices.flat})
    except Exception:
        width = 2
    return width if n % width == 0 else 1


def kernel(cfg, q_in, k_in, v_in, seg_ref, out_ref,
           q_ref, buf, segs, segcol, bias, acc, top, o_buf,
           kv_send, kv_recv, seg_send, seg_recv, o_send, o_recv, o_local):
    n, ny, reach, tp, groups, per_group, rows, head = cfg
    nz = n // ny
    depth = min(nz - 1, (reach + ny - 1) // ny) + 1
    out_rows = rows // tp
    const = math.log2(math.e) / math.sqrt(head)
    me = lax.axis_index("ctx")
    mt = lax.axis_index("tp")
    z = me // ny
    y = me % ny

    barrier = pltpu.get_barrier_semaphore()
    for d in range(1, reach + 1):
        @pl.when(me + d < n)
        def _():
            pl.semaphore_signal(barrier, inc=1, device_id={"ctx": me + d, "tp": mt}, device_id_type=MESH)

        @pl.when(me - d >= 0)
        def _():
            pl.semaphore_signal(barrier, inc=1, device_id={"ctx": me - d, "tp": mt}, device_id_type=MESH)
    for e in range(1, tp):
        pl.semaphore_signal(barrier, inc=1, device_id={"ctx": me, "tp": (mt + e) % tp}, device_id_type=MESH)
    peers = (tp - 1) + jnp.minimum(n - 1 - me, reach) + jnp.minimum(me, reach)
    pl.semaphore_wait(barrier, peers)

    def piece(s, dy, g, w):
        if s == 0 and dy == 0:
            return (k_in, v_in)[w].at[g]
        return buf.at[s * ny + dy, g, w]

    def sem_index(s, dy, g, w):
        return ((s * ny + dy) * groups + g) * 2 + w

    def send_index(s, e, g, w):
        return ((s * ny + e) * groups + g) * 2 + w

    def z_copy(s, g, w):
        return pltpu.make_async_remote_copy(
            src_ref=piece(s, 0, g, w),
            dst_ref=buf.at[(s + 1) * ny, g, w],
            send_sem=kv_send.at[send_index(s, 0, g, w)],
            recv_sem=kv_recv.at[sem_index(s + 1, 0, g, w)],
            device_id={"ctx": me + ny, "tp": mt},
            device_id_type=MESH,
        )

    def y_copy(s, e, g, w):
        return pltpu.make_async_remote_copy(
            src_ref=piece(s, 0, g, w),
            dst_ref=buf.at[s * ny + ny - e, g, w],
            send_sem=kv_send.at[send_index(s, e, g, w)],
            recv_sem=kv_recv.at[sem_index(s, ny - e, g, w)],
            device_id={"ctx": z * ny + (y + e) % ny, "tp": mt},
            device_id_type=MESH,
        )

    last = depth - 1
    straight = last >= 2 and last * ny > reach

    def far_copy(dy, g, w):
        return pltpu.make_async_remote_copy(
            src_ref=piece(last - 1, dy, g, w),
            dst_ref=buf.at[last * ny + dy, g, w],
            send_sem=kv_send.at[send_index(last, dy, g, w)],
            recv_sem=kv_recv.at[sem_index(last, dy, g, w)],
            device_id={"ctx": me + ny, "tp": mt},
            device_id_type=MESH,
        )

    def sends_far(dy):
        gap = me + ny - owner(last - 1, dy)
        return (z >= last - 1) & (z + 1 < nz) & (gap <= reach)

    def owner(s, dy):
        return (z - s) * ny + (y + dy) % ny

    def has_column(s):
        return (z >= s) & (s * ny <= reach)

    def sends_z(s):
        return (z >= s) & (z + 1 < nz) & ((s + 1) * ny <= reach)

    def sends_y(s, e):
        gap = z * ny + (y + e) % ny - owner(s, 0)
        return (z >= s) & (s * ny <= reach) & (gap > 0) & (gap <= reach)

    def wanted(s, dy):
        gap = me - owner(s, dy)
        return (z >= s) & (gap > 0) & (gap <= reach)

    def arrived(s, dy, g, w):
        pltpu.make_async_copy(buf.at[s * ny + dy, g, w], buf.at[s * ny + dy, g, w],
                              kv_recv.at[sem_index(s, dy, g, w)]).wait()

    def push(s, g):
        for w in range(2):
            if s > 0:
                @pl.when(has_column(s))
                def _():
                    arrived(s, 0, g, w)
            if s + 1 < depth:
                @pl.when(sends_z(s))
                def _():
                    z_copy(s, g, w).start()
            for e in range(1, ny):
                @pl.when(sends_y(s, e))
                def _():
                    y_copy(s, e, g, w).start()

    def seg_copy(d):
        return pltpu.make_async_remote_copy(
            src_ref=seg_ref,
            dst_ref=segs.at[d],
            send_sem=seg_send.at[d],
            recv_sem=seg_recv.at[d],
            device_id={"ctx": me + d, "tp": mt},
            device_id_type=MESH,
        )

    push(0, 0)
    for d in range(1, reach + 1):
        @pl.when(me + d < n)
        def _():
            seg_copy(d).start()

    for i in range(groups * per_group):
        q_ref[i] = q_in[:, i, :]
    segcol[...] = jnp.transpose(jnp.broadcast_to(seg_ref[...], (head, rows)))

    def attend(s, dy, g, first):
        k_ref, v_ref = piece(s, dy, g, 0), piece(s, dy, g, 1)
        if first:
            seg_k = seg_ref[...]
        else:
            seg_k = segs[me - owner(s, dy)]
        column = segcol[...]
        allowed = jnp.concatenate([column] * (rows // head), axis=1) == seg_k
        if first:
            r = lax.broadcasted_iota(jnp.int32, (rows, rows), 0)
            c = lax.broadcasted_iota(jnp.int32, (rows, rows), 1)
            allowed = allowed & (c <= r)
        bias[...] = jnp.where(allowed, 0.0, NEG)

        def one(h, carry):
            i = g * per_group + h
            scores = lax.dot_general(q_ref[i], k_ref[...], (((1,), (1,)), ((), ())),
                                     preferred_element_type=jnp.float32)
            scores = scores * const + bias[...]
            high = jnp.broadcast_to(jnp.max(scores, axis=1, keepdims=True), (rows, head))
            if not first:
                old = top[i]
                high = jnp.maximum(old, high)
            weights = jnp.exp2(scores - jnp.concatenate([high] * (rows // head), axis=1)).astype(jnp.bfloat16)
            v = jnp.concatenate([v_ref[...], jnp.ones((rows, head), jnp.bfloat16)], axis=1)
            mixed = jnp.dot(weights, v, preferred_element_type=jnp.float32)
            if not first:
                factor = jnp.exp2(old - high)
                mixed = acc[i] * jnp.concatenate([factor, factor], axis=1) + mixed
            acc[i] = mixed
            top[i] = high
            return carry

        lax.fori_loop(0, per_group, one, 0, unroll=per_group)

    def attend_y(s, g):
        for dy in range(1, ny):
            @pl.when(wanted(s, dy))
            def _():
                arrived(s, dy, g, 0)
                arrived(s, dy, g, 1)
                if straight and s == last - 1:
                    @pl.when(sends_far(dy))
                    def _():
                        far_copy(dy, g, 0).start()
                        far_copy(dy, g, 1).start()
                attend(s, dy, g, False)

    per_send = max(per_group // 2, 1)
    width = per_send * head
    pieces = per_group // per_send

    def o_copy(c, e):
        col = pl.multiple_of((mt * groups * pieces + c) * width, width)
        to = (mt + e) % tp
        return pltpu.make_async_remote_copy(
            src_ref=o_buf.at[pl.ds(pl.multiple_of(to * out_rows, out_rows), out_rows), pl.ds(c * width, width)],
            dst_ref=out_ref.at[:, pl.ds(col, width)],
            send_sem=o_send.at[c * tp + e],
            recv_sem=o_recv.at[c * tp + e],
            device_id={"ctx": me, "tp": to},
            device_id_type=MESH,
        )

    def o_own(c):
        col = pl.multiple_of((mt * groups * pieces + c) * width, width)
        return pltpu.make_async_copy(
            o_buf.at[pl.ds(pl.multiple_of(mt * out_rows, out_rows), out_rows), pl.ds(c * width, width)],
            out_ref.at[:, pl.ds(col, width)],
            o_local.at[c],
        )

    def finish(g):
        for p in range(pieces):
            c = g * pieces + p
            for h in range(per_send):
                i = g * per_group + p * per_send + h
                o_buf[:, i * head:(i + 1) * head] = (acc[i, :, :head] / acc[i, :, head:]).astype(jnp.bfloat16)
            for e in range(1, tp):
                o_copy(c, e).start()
            o_own(c).start()

    for g in range(groups):
        attend(0, 0, g, True)
        if g == 0:
            for d in range(1, reach + 1):
                @pl.when(me - d >= 0)
                def _():
                    pltpu.make_async_copy(segs.at[d], segs.at[d], seg_recv.at[d]).wait()
        for s in range(1, depth):
            push(s, g)
            if s == depth - 1 and g + 1 < groups:
                push(0, g + 1)

            @pl.when(wanted(s, 0))
            def _():
                attend(s, 0, g, False)
            attend_y(s - 1, g)
        if depth == 1 and g + 1 < groups:
            push(0, g + 1)
        attend_y(depth - 1, g)
        finish(g)

    for s in range(depth):
        for g in range(groups):
            for w in range(2):
                if s + 1 < depth:
                    @pl.when(sends_z(s))
                    def _():
                        z_copy(s, g, w).wait_send()
                for e in range(1, ny):
                    @pl.when(sends_y(s, e))
                    def _():
                        y_copy(s, e, g, w).wait_send()
    if straight:
        for g in range(groups):
            for w in range(2):
                for dy in range(1, ny):
                    @pl.when(wanted(last - 1, dy) & sends_far(dy))
                    def _():
                        far_copy(dy, g, w).wait_send()
    for d in range(1, reach + 1):
        @pl.when(me + d < n)
        def _():
            seg_copy(d).wait_send()
    for c in range(groups * pieces):
        o_own(c).wait()
        for e in range(1, tp):
            o_copy(c, e).wait()


def local(ny, queries, keys, values, segment_ids):
    rows, heads, head = queries.shape
    groups = keys.shape[1]
    per_group = heads // groups
    n = lax.axis_size("ctx")
    tp = lax.axis_size("tp")
    nz = n // ny
    longest = rows * n * 5 // 8
    reach = min((longest + rows - 1) // rows, n - 1)
    depth = min(nz - 1, (reach + ny - 1) // ny) + 1
    k = jnp.transpose(keys, (1, 0, 2))
    v = jnp.transpose(values, (1, 0, 2))
    pieces = groups * (per_group // max(per_group // 2, 1))
    slots = depth * ny
    vmem = pl.BlockSpec(memory_space=pltpu.VMEM)
    dma = pltpu.SemaphoreType.DMA
    cfg = (n, ny, reach, tp, groups, per_group, rows, head)
    return pl.pallas_call(
        functools.partial(kernel, cfg),
        out_shape=pltpu.VMEM((rows // tp, tp * heads * head), jnp.bfloat16),
        in_specs=[vmem] * 4,
        out_specs=vmem,
        scratch_shapes=[
            pltpu.VMEM((heads, rows, head), jnp.bfloat16),
            pltpu.VMEM((slots, groups, 2, rows, head), jnp.bfloat16),
            pltpu.VMEM((reach + 1, 1, rows), jnp.int32),
            pltpu.VMEM((rows, head), jnp.int32),
            pltpu.VMEM((rows, rows), jnp.float32),
            pltpu.VMEM((heads, rows, 2 * head), jnp.float32),
            pltpu.VMEM((heads, rows, head), jnp.float32),
            pltpu.VMEM((rows, heads * head), jnp.bfloat16),
            dma((slots * groups * 2,)),
            dma((slots * groups * 2,)),
            dma((reach + 1,)),
            dma((reach + 1,)),
            dma((pieces * tp,)),
            dma((pieces * tp,)),
            dma((pieces,)),
        ],
        compiler_params=pltpu.CompilerParams(
            collective_id=0, has_side_effects=True, vmem_limit_bytes=56 * 1024 * 1024
        ),
    )(queries, k, v, segment_ids.reshape(1, rows))


UNITS = (
    (0, 0, 0, 0, 0, 0, 0, 0),
    (0, 0, 0, 0, 0, 0, 0, 0),
    (0, 0, 48, 49, 50, 51, 52, 51),
    (0, 0, 0, 50, 51, 52, 50, 52),
    (0, 0, 0, 0, 48, 50, 53, 54),
    (0, 0, 0, 0, 0, 48, 51, 53),
    (0, 48, 49, 48, 49, 49, 49, 50),
    (0, 0, 25, 26, 26, 27, 26, 29),
    (0, 0, 0, 25, 24, 28, 29, 30),
    (0, 0, 0, 0, 25, 25, 28, 28),
    (0, 0, 0, 0, 0, 26, 27, 27),
    (0, 24, 24, 24, 27, 24, 25, 26),
)
EVENTS = (
    (
        (2144, 2081, 2146, 2091, 2148, 2101, 2126, 0),
        (2152, 2217, 2154, 2083, 2156, 2093, 2142, 0),
        (0, 0, 2170, 0, 2164, 2155, 2116, 0),
        (0, 0, 0, 0, 2154, 2085, 0, 0),
        (0, 0, 0, 0, 2146, 0, 0, 0),
    ),
    (
        (2160, 0, 0, 2273, 2170, 2060, 2124, 2133),
        (0, 0, 0, 2107, 2048, 0, 2118, 2125),
        (0, 0, 0, 2074, 0, 0, 0, 2123),
        (0, 0, 0, 0, 0, 0, 0, 2078),
    ),
    (
        (2168, 2105, 2144, 2169, 2120, 2147, 2122, 2117),
        (0, 0, 2152, 2099, 2172, 2109, 2114, 2052),
        (0, 0, 2162, 2050, 2081, 2171, 0, 2062),
        (0, 0, 2089, 2058, 0, 2049, 0, 2115),
        (0, 0, 0, 2080, 0, 2068, 0, 2054),
        (0, 0, 0, 2056, 0, 0, 0, 2060),
        (0, 0, 0, 2057, 0, 0, 0, 0),
        (0, 0, 0, 2161, 0, 0, 0, 0),
    ),
    (
        (0, 2097, 2049, 0, 2059, 2052, 2132, 0),
        (0, 0, 0, 0, 2153, 2137, 2061, 0),
        (0, 0, 0, 0, 2051, 2058, 2134, 0),
    ),
    (
        (0, 2048, 2168, 0, 2162, 2050, 2059, 0),
        (0, 0, 0, 0, 0, 2163, 2053, 0),
    ),
    (
        (0, 2056, 2160, 0, 0, 2048, 2074, 2141),
        (0, 0, 0, 0, 0, 2056, 2140, 2139),
        (0, 0, 0, 0, 0, 2106, 2049, 2050),
        (0, 0, 0, 0, 0, 0, 2051, 0),
    ),
    (
        (0, 0, 0, 0, 0, 2057, 2057, 2058),
    ),
    (
        (0, 2064, 2097, 2096, 2105, 2076, 2130, 2131),
        (0, 0, 2073, 2066, 2072, 2064, 2069, 2070),
        (0, 0, 0, 2104, 2097, 0, 0, 2068),
    ),
    (
        (0, 2072, 0, 0, 2064, 2065, 2077, 0),
        (0, 0, 0, 0, 2067, 0, 0, 0),
        (0, 0, 0, 0, 2075, 0, 0, 0),
    ),
    (
        (0, 0, 0, 0, 0, 2072, 0, 2076),
        (0, 0, 0, 0, 0, 2066, 0, 0),
    ),
    (
        (0, 0, 0, 0, 0, 0, 2065, 2074),
        (0, 0, 0, 0, 0, 0, 2075, 0),
        (0, 0, 0, 0, 0, 0, 2073, 0),
        (0, 0, 0, 0, 0, 0, 2067, 0),
    ),
    (
        (0, 0, 0, 0, 0, 0, 0, 2066),
    ),
    (),
)
LAST = (6, 11)


def targets(code, me):
    found = []
    if code // 2048 % 2:
        if code // 32 % 2:
            found.append(me + 2)
        if code // 64 % 2:
            found.append(me ^ 1)
        if code // 128 % 8:
            found.append(me + code // 128 % 8)
    return found


def planned_kernel(cfg, q_hbm, k_hbm, v_hbm, seg_hbm, out_ref,
                   q_raw, kv_raw, q_ref, buf, segs, segcol, bias, acc, top, o_buf,
                   load, kv_send, kv_recv, seg_send, seg_recv, o_send, o_recv):
    n, tp, groups, per_group, rows, head = cfg
    out_rows = rows // tp
    const = math.log2(math.e) / math.sqrt(head)
    me = lax.axis_index("ctx")
    mt = lax.axis_index("tp")

    def pick(values):
        usual = max(set(values), key=values.count)
        chosen = jnp.int32(usual)
        for d, value in enumerate(values):
            if value != usual:
                chosen = jnp.where(me == d, jnp.int32(value), chosen)
        return chosen

    k_load = pltpu.make_async_copy(k_hbm, kv_raw.at[0], load.at[0])
    v_load = pltpu.make_async_copy(v_hbm, kv_raw.at[1], load.at[1])
    seg_load = pltpu.make_async_copy(seg_hbm, segs.at[me], load.at[2])
    q_load = pltpu.make_async_copy(q_hbm, q_raw, load.at[3])
    k_load.start()
    v_load.start()
    seg_load.start()
    q_load.start()

    edges = sorted({(m, t) for step in EVENTS for slot in step for m, code in enumerate(slot) for t in targets(code, m)})
    barrier = pltpu.get_barrier_semaphore()
    for s, d in edges:
        @pl.when(me == d)
        def _():
            pl.semaphore_signal(barrier, inc=1, device_id={"ctx": s, "tp": mt}, device_id_type=MESH)
    for e in range(1, tp):
        pl.semaphore_signal(barrier, inc=1, device_id={"ctx": me, "tp": (mt + e) % tp}, device_id_type=MESH)
    k_load.wait()
    v_load.wait()
    for w in range(2):
        for g in range(groups):
            buf[me, g, w] = kv_raw[w, :, g, :]
    seg_load.wait()
    pl.semaphore_wait(barrier, pick([sum(s == m for s, _ in edges) for m in range(n)]) + (tp - 1))

    def piece_copy(b, gw, way, to):
        index = b * (2 * groups) + gw
        return pltpu.make_async_remote_copy(
            src_ref=buf.at[b, gw // 2, gw % 2],
            dst_ref=buf.at[b, gw // 2, gw % 2],
            send_sem=kv_send.at[index * 3 + way],
            recv_sem=kv_recv.at[index],
            device_id={"ctx": to, "tp": mt},
            device_id_type=MESH,
        )

    def seg_copy(b, way, to):
        return pltpu.make_async_remote_copy(
            src_ref=segs.at[b],
            dst_ref=segs.at[b],
            send_sem=seg_send.at[b * 3 + way],
            recv_sem=seg_recv.at[b],
            device_id={"ctx": to, "tp": mt},
            device_id_type=MESH,
        )

    def routes(slot):
        code = pick(slot)
        b, gw, far = code % 8, code // 8 % 4, code // 128 % 8
        ways = []
        if any(v // 32 % 2 for v in slot):
            ways.append((0, code // 32 % 2 == 1, me + 2))
        if any(v // 64 % 2 for v in slot):
            ways.append((1, code // 64 % 2 == 1, me + 1 - 2 * (me % 2)))
        if any(v // 128 % 8 for v in slot):
            ways.append((2, far > 0, me + far))
        return code, b, gw, ways

    def event(slot):
        code, b, gw, ways = routes(slot)
        head_piece = any(v // 2048 and v // 8 % 4 == 0 for v in slot)

        @pl.when(code // 2048 == 1)
        def _():
            @pl.when(b != me)
            def _():
                pltpu.make_async_copy(buf.at[b, gw // 2, gw % 2], buf.at[b, gw // 2, gw % 2],
                                      kv_recv.at[b * (2 * groups) + gw]).wait()
            for way, on, to in ways:
                @pl.when(on)
                def _():
                    piece_copy(b, gw, way, to).start()
            if head_piece:
                @pl.when(gw == 0)
                def _():
                    @pl.when(b != me)
                    def _():
                        pltpu.make_async_copy(segs.at[b], segs.at[b], seg_recv.at[b]).wait()
                    for way, on, to in ways:
                        @pl.when(on)
                        def _():
                            seg_copy(b, way, to).start()

    def drain(slot):
        code, b, gw, ways = routes(slot)
        head_piece = any(v // 2048 and v // 8 % 4 == 0 for v in slot)

        @pl.when(code // 2048 == 1)
        def _():
            for way, on, to in ways:
                @pl.when(on)
                def _():
                    piece_copy(b, gw, way, to).wait_send()
            if head_piece:
                @pl.when(gw == 0)
                def _():
                    for way, on, to in ways:
                        @pl.when(on)
                        def _():
                            seg_copy(b, way, to).wait_send()

    def several(b, g, hs, first):
        count = len(hs)
        span = pl.ds(g * per_group + hs[0], count)
        scores = lax.dot_general(q_ref[span].reshape(count * rows, head), buf[b, g, 0], (((1,), (1,)), ((), ())),
                                 preferred_element_type=jnp.float32)
        scores = scores * const + jnp.concatenate([bias[...]] * count, axis=0)
        high = jnp.broadcast_to(jnp.max(scores, axis=1, keepdims=True), (count * rows, head))
        if not first:
            old = top[span].reshape(count * rows, head)
            high = jnp.maximum(old, high)
        weights = jnp.exp2(scores - jnp.concatenate([high] * (rows // head), axis=1)).astype(jnp.bfloat16)
        v = jnp.concatenate([buf[b, g, 1], jnp.ones((rows, head), jnp.bfloat16)], axis=1)
        mixed = jnp.dot(weights, v, preferred_element_type=jnp.float32)
        if not first:
            factor = jnp.exp2(old - high)
            mixed = acc[span].reshape(count * rows, 2 * head) * jnp.concatenate([factor, factor], axis=1) + mixed
        acc[span] = mixed.reshape(count, rows, 2 * head)
        top[span] = high.reshape(count, rows, head)

    def set_bias(b, first):
        allowed = jnp.concatenate([segcol[...]] * (rows // head), axis=1) == segs[b]
        if first:
            r = lax.broadcasted_iota(jnp.int32, (rows, rows), 0)
            c = lax.broadcasted_iota(jnp.int32, (rows, rows), 1)
            allowed = allowed & (c <= r)
        bias[...] = jnp.where(allowed, 0.0, NEG)

    def unit(values):
        code = pick(values)
        b, g = code % 8, code // 8 % 2

        @pl.when(code // 16 % 2 == 1)
        def _():
            set_bias(b, False)
            several(b, g, range(per_group), False)

    per_send = per_group // 2
    width = per_send * head
    pieces = per_group // per_send

    def o_copy(c, e):
        col = pl.multiple_of((mt * groups * pieces + c) * width, width)
        to = (mt + e) % tp
        return pltpu.make_async_remote_copy(
            src_ref=o_buf.at[pl.ds(pl.multiple_of(to * out_rows, out_rows), out_rows), pl.ds(c * width, width)],
            dst_ref=out_ref.at[:, pl.ds(col, width)],
            send_sem=o_send.at[c * tp + e],
            recv_sem=o_recv.at[c * tp + e],
            device_id={"ctx": me, "tp": to},
            device_id_type=MESH,
        )

    def last_unit(values, g):
        code = pick(values)
        b = code % 8
        live = code // 16 % 2 == 1

        @pl.when(live)
        def _():
            set_bias(b, False)
        for p in range(pieces):
            @pl.when(live)
            def _():
                several(b, g, range(p * per_send, (p + 1) * per_send), False)
            c = g * pieces + p
            for h in range(per_send):
                i = g * per_group + p * per_send + h
                o_buf[:, i * head:(i + 1) * head] = (acc[i, :, :head] / acc[i, :, head:]).astype(jnp.bfloat16)
            for e in range(1, tp):
                o_copy(c, e).start()
            mine = pl.ds(pl.multiple_of(mt * out_rows, out_rows), out_rows)
            col = pl.multiple_of((mt * groups * pieces + c) * width, width)
            out_ref[:, pl.ds(col, width)] = o_buf[mine, c * width:(c + 1) * width]

    for slot in EVENTS[0]:
        event(slot)
    q_load.wait()
    segcol[...] = jnp.transpose(jnp.broadcast_to(segs[me], (head, rows)))
    set_bias(me, True)
    for step, values in enumerate(UNITS):
        if step > 0:
            for slot in EVENTS[step]:
                event(slot)
        if step < groups:
            for h in range(step * per_group, (step + 1) * per_group):
                q_ref[h] = q_raw[:, h, :]
            several(me, step, range(per_group), True)
        elif step in LAST:
            last_unit(values, LAST.index(step))
        else:
            unit(values)
    for slot in EVENTS[len(UNITS)]:
        event(slot)

    for group in EVENTS:
        for slot in group:
            drain(slot)
    for c in range(groups * pieces):
        for e in range(1, tp):
            o_copy(c, e).wait()


def planned(queries, keys, values, segment_ids):
    rows, heads, head = queries.shape
    groups = keys.shape[1]
    per_group = heads // groups
    n = lax.axis_size("ctx")
    tp = lax.axis_size("tp")
    chunks = groups * 2
    hbm = pl.BlockSpec(memory_space=pltpu.HBM)
    dma = pltpu.SemaphoreType.DMA
    cfg = (n, tp, groups, per_group, rows, head)
    return pl.pallas_call(
        functools.partial(planned_kernel, cfg),
        out_shape=pltpu.VMEM((rows // tp, tp * heads * head), jnp.bfloat16),
        in_specs=[hbm] * 4,
        out_specs=pl.BlockSpec(memory_space=pltpu.VMEM),
        scratch_shapes=[
            pltpu.VMEM((rows, heads, head), jnp.bfloat16),
            pltpu.VMEM((2, rows, groups, head), jnp.bfloat16),
            pltpu.VMEM((heads, rows, head), jnp.bfloat16),
            pltpu.VMEM((n, groups, 2, rows, head), jnp.bfloat16),
            pltpu.VMEM((n, 1, rows), jnp.int32),
            pltpu.VMEM((rows, head), jnp.int32),
            pltpu.VMEM((rows, rows), jnp.float32),
            pltpu.VMEM((heads, rows, 2 * head), jnp.float32),
            pltpu.VMEM((heads, rows, head), jnp.float32),
            pltpu.VMEM((rows, heads * head), jnp.bfloat16),
            dma((4,)),
            dma((n * groups * 2 * 3,)),
            dma((n * groups * 2,)),
            dma((n * 3,)),
            dma((n,)),
            dma((chunks * tp,)),
            dma((chunks * tp,)),
        ],
        compiler_params=pltpu.CompilerParams(
            collective_id=0, has_side_effects=True, vmem_limit_bytes=56 * 1024 * 1024
        ),
    )(queries, keys, values, segment_ids.reshape(1, rows))


def fits_plan(mesh):
    n = mesh.shape["ctx"]
    return plane_width(mesh) == 2 and n == len(UNITS[0])


def solution(mesh):
    in_specs = (P("ctx", "tp", None), P("ctx", "tp", None), P("ctx", "tp", None), P("ctx"))
    out_specs = P(("ctx", "tp"), None)
    body = planned if fits_plan(mesh) else functools.partial(local, plane_width(mesh))
    return jax.shard_map(body, mesh=mesh, in_specs=in_specs, out_specs=out_specs, check_vma=False)
```

```python
import functools
import math

import jax
import jax.numpy as jnp
from jax import lax
from jax.experimental import pallas as pl
from jax.experimental.pallas import tpu as pltpu
from jax.sharding import PartitionSpec as P

MESH = pl.DeviceIdType.MESH
NEG = -1e30


def plane_width(mesh):
    n = mesh.shape["ctx"]
    try:
        width = len({d.coords[1] for d in mesh.devices.flat})
    except Exception:
        width = 2
    return width if n % width == 0 else 1


def kernel(cfg, q_in, k_in, v_in, seg_ref, out_ref,
           q_ref, buf, segs, segcol, bias, acc, top, o_buf,
           kv_send, kv_recv, seg_send, seg_recv, o_send, o_recv, o_local):
    n, ny, reach, tp, groups, per_group, rows, head = cfg
    nz = n // ny
    depth = min(nz - 1, (reach + ny - 1) // ny) + 1
    out_rows = rows // tp
    const = math.log2(math.e) / math.sqrt(head)
    me = lax.axis_index("ctx")
    mt = lax.axis_index("tp")
    z = me // ny
    y = me % ny

    barrier = pltpu.get_barrier_semaphore()
    for d in range(1, reach + 1):
        @pl.when(me + d < n)
        def _():
            pl.semaphore_signal(barrier, inc=1, device_id={"ctx": me + d, "tp": mt}, device_id_type=MESH)

        @pl.when(me - d >= 0)
        def _():
            pl.semaphore_signal(barrier, inc=1, device_id={"ctx": me - d, "tp": mt}, device_id_type=MESH)
    for e in range(1, tp):
        pl.semaphore_signal(barrier, inc=1, device_id={"ctx": me, "tp": (mt + e) % tp}, device_id_type=MESH)
    peers = (tp - 1) + jnp.minimum(n - 1 - me, reach) + jnp.minimum(me, reach)
    pl.semaphore_wait(barrier, peers)

    def piece(s, dy, g, w):
        if s == 0 and dy == 0:
            return (k_in, v_in)[w].at[g]
        return buf.at[s * ny + dy, g, w]

    def sem_index(s, dy, g, w):
        return ((s * ny + dy) * groups + g) * 2 + w

    def send_index(s, e, g, w):
        return ((s * ny + e) * groups + g) * 2 + w

    def z_copy(s, g, w):
        return pltpu.make_async_remote_copy(
            src_ref=piece(s, 0, g, w),
            dst_ref=buf.at[(s + 1) * ny, g, w],
            send_sem=kv_send.at[send_index(s, 0, g, w)],
            recv_sem=kv_recv.at[sem_index(s + 1, 0, g, w)],
            device_id={"ctx": me + ny, "tp": mt},
            device_id_type=MESH,
        )

    def y_copy(s, e, g, w):
        return pltpu.make_async_remote_copy(
            src_ref=piece(s, 0, g, w),
            dst_ref=buf.at[s * ny + ny - e, g, w],
            send_sem=kv_send.at[send_index(s, e, g, w)],
            recv_sem=kv_recv.at[sem_index(s, ny - e, g, w)],
            device_id={"ctx": z * ny + (y + e) % ny, "tp": mt},
            device_id_type=MESH,
        )

    last = depth - 1
    straight = last >= 2 and last * ny > reach

    def far_copy(dy, g, w):
        return pltpu.make_async_remote_copy(
            src_ref=piece(last - 1, dy, g, w),
            dst_ref=buf.at[last * ny + dy, g, w],
            send_sem=kv_send.at[send_index(last, dy, g, w)],
            recv_sem=kv_recv.at[sem_index(last, dy, g, w)],
            device_id={"ctx": me + ny, "tp": mt},
            device_id_type=MESH,
        )

    def sends_far(dy):
        gap = me + ny - owner(last - 1, dy)
        return (z >= last - 1) & (z + 1 < nz) & (gap <= reach)

    def owner(s, dy):
        return (z - s) * ny + (y + dy) % ny

    def has_column(s):
        return (z >= s) & (s * ny <= reach)

    def sends_z(s):
        return (z >= s) & (z + 1 < nz) & ((s + 1) * ny <= reach)

    def sends_y(s, e):
        gap = z * ny + (y + e) % ny - owner(s, 0)
        return (z >= s) & (s * ny <= reach) & (gap > 0) & (gap <= reach)

    def wanted(s, dy):
        gap = me - owner(s, dy)
        return (z >= s) & (gap > 0) & (gap <= reach)

    def arrived(s, dy, g, w):
        pltpu.make_async_copy(buf.at[s * ny + dy, g, w], buf.at[s * ny + dy, g, w],
                              kv_recv.at[sem_index(s, dy, g, w)]).wait()

    def push(s, g):
        for w in range(2):
            if s > 0:
                @pl.when(has_column(s))
                def _():
                    arrived(s, 0, g, w)
            if s + 1 < depth:
                @pl.when(sends_z(s))
                def _():
                    z_copy(s, g, w).start()
            for e in range(1, ny):
                @pl.when(sends_y(s, e))
                def _():
                    y_copy(s, e, g, w).start()

    def seg_copy(d):
        return pltpu.make_async_remote_copy(
            src_ref=seg_ref,
            dst_ref=segs.at[d],
            send_sem=seg_send.at[d],
            recv_sem=seg_recv.at[d],
            device_id={"ctx": me + d, "tp": mt},
            device_id_type=MESH,
        )

    push(0, 0)
    for d in range(1, reach + 1):
        @pl.when(me + d < n)
        def _():
            seg_copy(d).start()

    for i in range(groups * per_group):
        q_ref[i] = q_in[:, i, :]
    segcol[...] = jnp.transpose(jnp.broadcast_to(seg_ref[...], (head, rows)))

    def attend(s, dy, g, first):
        k_ref, v_ref = piece(s, dy, g, 0), piece(s, dy, g, 1)
        if first:
            seg_k = seg_ref[...]
        else:
            seg_k = segs[me - owner(s, dy)]
        column = segcol[...]
        allowed = jnp.concatenate([column] * (rows // head), axis=1) == seg_k
        if first:
            r = lax.broadcasted_iota(jnp.int32, (rows, rows), 0)
            c = lax.broadcasted_iota(jnp.int32, (rows, rows), 1)
            allowed = allowed & (c <= r)
        bias[...] = jnp.where(allowed, 0.0, NEG)

        def one(h, carry):
            i = g * per_group + h
            scores = lax.dot_general(q_ref[i], k_ref[...], (((1,), (1,)), ((), ())),
                                     preferred_element_type=jnp.float32)
            scores = scores * const + bias[...]
            high = jnp.broadcast_to(jnp.max(scores, axis=1, keepdims=True), (rows, head))
            if not first:
                old = top[i]
                high = jnp.maximum(old, high)
            weights = jnp.exp2(scores - jnp.concatenate([high] * (rows // head), axis=1)).astype(jnp.bfloat16)
            v = jnp.concatenate([v_ref[...], jnp.ones((rows, head), jnp.bfloat16)], axis=1)
            mixed = jnp.dot(weights, v, preferred_element_type=jnp.float32)
            if not first:
                factor = jnp.exp2(old - high)
                mixed = acc[i] * jnp.concatenate([factor, factor], axis=1) + mixed
            acc[i] = mixed
            top[i] = high
            return carry

        lax.fori_loop(0, per_group, one, 0, unroll=per_group)

    def attend_y(s, g):
        for dy in range(1, ny):
            @pl.when(wanted(s, dy))
            def _():
                arrived(s, dy, g, 0)
                arrived(s, dy, g, 1)
                if straight and s == last - 1:
                    @pl.when(sends_far(dy))
                    def _():
                        far_copy(dy, g, 0).start()
                        far_copy(dy, g, 1).start()
                attend(s, dy, g, False)

    per_send = max(per_group // 2, 1)
    width = per_send * head
    pieces = per_group // per_send

    def o_copy(c, e):
        col = pl.multiple_of((mt * groups * pieces + c) * width, width)
        to = (mt + e) % tp
        return pltpu.make_async_remote_copy(
            src_ref=o_buf.at[pl.ds(pl.multiple_of(to * out_rows, out_rows), out_rows), pl.ds(c * width, width)],
            dst_ref=out_ref.at[:, pl.ds(col, width)],
            send_sem=o_send.at[c * tp + e],
            recv_sem=o_recv.at[c * tp + e],
            device_id={"ctx": me, "tp": to},
            device_id_type=MESH,
        )

    def o_own(c):
        col = pl.multiple_of((mt * groups * pieces + c) * width, width)
        return pltpu.make_async_copy(
            o_buf.at[pl.ds(pl.multiple_of(mt * out_rows, out_rows), out_rows), pl.ds(c * width, width)],
            out_ref.at[:, pl.ds(col, width)],
            o_local.at[c],
        )

    def finish(g):
        for p in range(pieces):
            c = g * pieces + p
            for h in range(per_send):
                i = g * per_group + p * per_send + h
                o_buf[:, i * head:(i + 1) * head] = (acc[i, :, :head] / acc[i, :, head:]).astype(jnp.bfloat16)
            for e in range(1, tp):
                o_copy(c, e).start()
            o_own(c).start()

    for g in range(groups):
        attend(0, 0, g, True)
        if g == 0:
            for d in range(1, reach + 1):
                @pl.when(me - d >= 0)
                def _():
                    pltpu.make_async_copy(segs.at[d], segs.at[d], seg_recv.at[d]).wait()
        for s in range(1, depth):
            push(s, g)
            if s == depth - 1 and g + 1 < groups:
                push(0, g + 1)

            @pl.when(wanted(s, 0))
            def _():
                attend(s, 0, g, False)
            attend_y(s - 1, g)
        if depth == 1 and g + 1 < groups:
            push(0, g + 1)
        attend_y(depth - 1, g)
        finish(g)

    for s in range(depth):
        for g in range(groups):
            for w in range(2):
                if s + 1 < depth:
                    @pl.when(sends_z(s))
                    def _():
                        z_copy(s, g, w).wait_send()
                for e in range(1, ny):
                    @pl.when(sends_y(s, e))
                    def _():
                        y_copy(s, e, g, w).wait_send()
    if straight:
        for g in range(groups):
            for w in range(2):
                for dy in range(1, ny):
                    @pl.when(wanted(last - 1, dy) & sends_far(dy))
                    def _():
                        far_copy(dy, g, w).wait_send()
    for d in range(1, reach + 1):
        @pl.when(me + d < n)
        def _():
            seg_copy(d).wait_send()
    for c in range(groups * pieces):
        o_own(c).wait()
        for e in range(1, tp):
            o_copy(c, e).wait()


def local(ny, queries, keys, values, segment_ids):
    rows, heads, head = queries.shape
    groups = keys.shape[1]
    per_group = heads // groups
    n = lax.axis_size("ctx")
    tp = lax.axis_size("tp")
    nz = n // ny
    longest = rows * n * 5 // 8
    reach = min((longest + rows - 1) // rows, n - 1)
    depth = min(nz - 1, (reach + ny - 1) // ny) + 1
    k = jnp.transpose(keys, (1, 0, 2))
    v = jnp.transpose(values, (1, 0, 2))
    pieces = groups * (per_group // max(per_group // 2, 1))
    slots = depth * ny
    vmem = pl.BlockSpec(memory_space=pltpu.VMEM)
    dma = pltpu.SemaphoreType.DMA
    cfg = (n, ny, reach, tp, groups, per_group, rows, head)
    return pl.pallas_call(
        functools.partial(kernel, cfg),
        out_shape=pltpu.VMEM((rows // tp, tp * heads * head), jnp.bfloat16),
        in_specs=[vmem] * 4,
        out_specs=vmem,
        scratch_shapes=[
            pltpu.VMEM((heads, rows, head), jnp.bfloat16),
            pltpu.VMEM((slots, groups, 2, rows, head), jnp.bfloat16),
            pltpu.VMEM((reach + 1, 1, rows), jnp.int32),
            pltpu.VMEM((rows, head), jnp.int32),
            pltpu.VMEM((rows, rows), jnp.float32),
            pltpu.VMEM((heads, rows, 2 * head), jnp.float32),
            pltpu.VMEM((heads, rows, head), jnp.float32),
            pltpu.VMEM((rows, heads * head), jnp.bfloat16),
            dma((slots * groups * 2,)),
            dma((slots * groups * 2,)),
            dma((reach + 1,)),
            dma((reach + 1,)),
            dma((pieces * tp,)),
            dma((pieces * tp,)),
            dma((pieces,)),
        ],
        compiler_params=pltpu.CompilerParams(
            collective_id=0, has_side_effects=True, vmem_limit_bytes=56 * 1024 * 1024
        ),
    )(queries, k, v, segment_ids.reshape(1, rows))


UNITS = (
    (0, 0, 0, 0, 0, 0, 0, 0),
    (0, 0, 0, 0, 0, 0, 0, 0),
    (0, 0, 49, 50, 49, 51, 52, 53),
    (0, 0, 0, 57, 51, 50, 50, 51),
    (0, 0, 0, 17, 50, 52, 53, 54),
    (0, 0, 0, 0, 0, 27, 51, 52),
    (0, 0, 0, 0, 0, 49, 0, 0),
    (0, 48, 48, 48, 48, 48, 49, 50),
    (0, 0, 24, 26, 26, 26, 29, 27),
    (0, 0, 0, 0, 25, 25, 28, 29),
    (0, 0, 0, 0, 24, 24, 26, 28),
    (0, 0, 0, 0, 0, 0, 27, 30),
    (0, 24, 25, 24, 27, 28, 25, 26),
)
EVENTS = (
    (
        (2144, 2081, 2154, 2083, 2156, 2085, 2118, 0),
        (2152, 2217, 2146, 2091, 2148, 2093, 2134, 0),
        (0, 0, 0, 0, 2164, 2147, 0, 0),
        (0, 0, 0, 0, 2154, 2155, 0, 0),
        (0, 0, 0, 0, 2146, 0, 0, 0),
        (0, 0, 0, 0, 2170, 0, 0, 0),
        (0, 0, 0, 0, 2172, 0, 0, 0),
    ),
    (
        (2168, 0, 2170, 2273, 0, 2060, 2126, 0),
        (0, 0, 0, 2107, 0, 2101, 2116, 0),
        (0, 0, 0, 2050, 0, 2109, 2124, 0),
        (0, 0, 0, 2057, 0, 0, 0, 0),
    ),
    (
        (2160, 2105, 2152, 2058, 2153, 2052, 2122, 2117),
        (0, 0, 2144, 2169, 2081, 0, 2114, 2054),
        (0, 0, 2089, 2099, 2048, 0, 0, 2125),
        (0, 0, 2162, 2074, 2120, 0, 0, 2115),
        (0, 0, 2049, 2161, 0, 0, 0, 2070),
        (0, 0, 0, 2056, 0, 0, 0, 2123),
        (0, 0, 0, 0, 0, 0, 0, 2052),
    ),
    (
        (0, 2056, 0, 0, 2059, 2171, 2132, 2062),
        (0, 0, 0, 0, 2051, 2058, 2053, 0),
        (0, 0, 0, 0, 0, 2050, 0, 0),
    ),
    (
        (0, 2048, 0, 2080, 2162, 2137, 2061, 2133),
        (0, 0, 0, 0, 0, 0, 2051, 0),
        (0, 0, 0, 0, 0, 0, 2142, 0),
        (0, 0, 0, 0, 0, 0, 2140, 0),
    ),
    (
        (0, 0, 0, 0, 0, 2163, 2074, 2141),
        (0, 0, 0, 0, 0, 0, 2059, 2060),
        (0, 0, 0, 0, 0, 0, 0, 2058),
    ),
    (
        (0, 0, 0, 0, 0, 2106, 2057, 2050),
        (0, 0, 0, 0, 0, 2068, 2069, 0),
        (0, 0, 0, 0, 0, 2049, 0, 0),
        (0, 0, 0, 0, 0, 2057, 0, 0),
    ),
    (
        (0, 0, 0, 0, 0, 2065, 2049, 0),
        (0, 0, 0, 0, 0, 2076, 0, 0),
        (0, 0, 0, 0, 0, 2048, 0, 0),
        (0, 0, 0, 0, 0, 2056, 0, 0),
    ),
    (
        (0, 2097, 2168, 2104, 2064, 2066, 2077, 2139),
        (0, 0, 2073, 2066, 2105, 0, 2130, 2131),
        (0, 0, 2160, 2096, 0, 0, 0, 2078),
        (0, 0, 2097, 0, 0, 0, 0, 0),
    ),
    (
        (0, 2072, 0, 0, 2097, 0, 0, 0),
        (0, 0, 0, 0, 2072, 0, 0, 0),
        (0, 0, 0, 0, 2075, 0, 0, 0),
    ),
    (
        (0, 2064, 0, 0, 2067, 2072, 0, 2068),
        (0, 0, 0, 0, 0, 2064, 0, 2076),
    ),
    (
        (0, 0, 0, 0, 0, 0, 2075, 2074),
        (0, 0, 0, 0, 0, 0, 2073, 0),
        (0, 0, 0, 0, 0, 0, 2067, 0),
        (0, 0, 0, 0, 0, 0, 2065, 0),
    ),
    (
        (0, 0, 0, 0, 0, 0, 0, 2066),
    ),
    (),
)
LAST = (7, 12)


def targets(code, me):
    found = []
    if code // 2048 % 2:
        if code // 32 % 2:
            found.append(me + 2)
        if code // 64 % 2:
            found.append(me ^ 1)
        if code // 128 % 8:
            found.append(me + code // 128 % 8)
    return found


def planned_kernel(cfg, q_hbm, k_hbm, v_hbm, seg_hbm, out_ref,
                   q_raw, kv_raw, q_ref, buf, segs, segcol, bias, acc, top, o_buf,
                   load, kv_send, kv_recv, seg_send, seg_recv, o_send, o_recv):
    n, tp, groups, per_group, rows, head = cfg
    out_rows = rows // tp
    const = math.log2(math.e) / math.sqrt(head)
    me = lax.axis_index("ctx")
    mt = lax.axis_index("tp")

    def pick(values):
        usual = max(set(values), key=values.count)
        chosen = jnp.int32(usual)
        for d, value in enumerate(values):
            if value != usual:
                chosen = jnp.where(me == d, jnp.int32(value), chosen)
        return chosen

    k_load = pltpu.make_async_copy(k_hbm, kv_raw.at[0], load.at[0])
    v_load = pltpu.make_async_copy(v_hbm, kv_raw.at[1], load.at[1])
    seg_load = pltpu.make_async_copy(seg_hbm, segs.at[me], load.at[2])
    q_load = pltpu.make_async_copy(q_hbm, q_raw, load.at[3])
    k_load.start()
    v_load.start()
    seg_load.start()
    q_load.start()

    edges = sorted({(m, t) for step in EVENTS for slot in step for m, code in enumerate(slot) for t in targets(code, m)})
    barrier = pltpu.get_barrier_semaphore()
    for s, d in edges:
        @pl.when(me == d)
        def _():
            pl.semaphore_signal(barrier, inc=1, device_id={"ctx": s, "tp": mt}, device_id_type=MESH)
    for e in range(1, tp):
        pl.semaphore_signal(barrier, inc=1, device_id={"ctx": me, "tp": (mt + e) % tp}, device_id_type=MESH)
    k_load.wait()
    v_load.wait()
    for w in range(2):
        for g in range(groups):
            buf[me, g, w] = kv_raw[w, :, g, :]
    seg_load.wait()
    pl.semaphore_wait(barrier, pick([sum(s == m for s, _ in edges) for m in range(n)]) + (tp - 1))

    def piece_copy(b, gw, way, to):
        index = b * (2 * groups) + gw
        return pltpu.make_async_remote_copy(
            src_ref=buf.at[b, gw // 2, gw % 2],
            dst_ref=buf.at[b, gw // 2, gw % 2],
            send_sem=kv_send.at[index * 3 + way],
            recv_sem=kv_recv.at[index],
            device_id={"ctx": to, "tp": mt},
            device_id_type=MESH,
        )

    def seg_copy(b, way, to):
        return pltpu.make_async_remote_copy(
            src_ref=segs.at[b],
            dst_ref=segs.at[b],
            send_sem=seg_send.at[b * 3 + way],
            recv_sem=seg_recv.at[b],
            device_id={"ctx": to, "tp": mt},
            device_id_type=MESH,
        )

    def routes(slot):
        code = pick(slot)
        b, gw, far = code % 8, code // 8 % 4, code // 128 % 8
        ways = []
        if any(v // 32 % 2 for v in slot):
            ways.append((0, code // 32 % 2 == 1, me + 2))
        if any(v // 64 % 2 for v in slot):
            ways.append((1, code // 64 % 2 == 1, me + 1 - 2 * (me % 2)))
        if any(v // 128 % 8 for v in slot):
            ways.append((2, far > 0, me + far))
        return code, b, gw, ways

    def event(slot):
        code, b, gw, ways = routes(slot)
        head_piece = any(v // 2048 and v // 8 % 4 == 0 for v in slot)

        @pl.when(code // 2048 == 1)
        def _():
            @pl.when(b != me)
            def _():
                pltpu.make_async_copy(buf.at[b, gw // 2, gw % 2], buf.at[b, gw // 2, gw % 2],
                                      kv_recv.at[b * (2 * groups) + gw]).wait()
            for way, on, to in ways:
                @pl.when(on)
                def _():
                    piece_copy(b, gw, way, to).start()
            if head_piece:
                @pl.when(gw == 0)
                def _():
                    @pl.when(b != me)
                    def _():
                        pltpu.make_async_copy(segs.at[b], segs.at[b], seg_recv.at[b]).wait()
                    for way, on, to in ways:
                        @pl.when(on)
                        def _():
                            seg_copy(b, way, to).start()

    def drain(slot):
        code, b, gw, ways = routes(slot)
        head_piece = any(v // 2048 and v // 8 % 4 == 0 for v in slot)

        @pl.when(code // 2048 == 1)
        def _():
            for way, on, to in ways:
                @pl.when(on)
                def _():
                    piece_copy(b, gw, way, to).wait_send()
            if head_piece:
                @pl.when(gw == 0)
                def _():
                    for way, on, to in ways:
                        @pl.when(on)
                        def _():
                            seg_copy(b, way, to).wait_send()

    def several(b, g, hs, first):
        count = len(hs)
        span = pl.ds(g * per_group + hs[0], count)
        scores = lax.dot_general(q_ref[span].reshape(count * rows, head), buf[b, g, 0], (((1,), (1,)), ((), ())),
                                 preferred_element_type=jnp.float32)
        scores = scores * const + jnp.concatenate([bias[b]] * count, axis=0)
        high = jnp.broadcast_to(jnp.max(scores, axis=1, keepdims=True), (count * rows, head))
        if not first:
            old = top[span].reshape(count * rows, head)
            high = jnp.maximum(old, high)
        weights = jnp.exp2(scores - jnp.concatenate([high] * (rows // head), axis=1)).astype(jnp.bfloat16)
        v = jnp.concatenate([buf[b, g, 1], jnp.ones((rows, head), jnp.bfloat16)], axis=1)
        mixed = jnp.dot(weights, v, preferred_element_type=jnp.float32)
        if not first:
            factor = jnp.exp2(old - high)
            mixed = acc[span].reshape(count * rows, 2 * head) * jnp.concatenate([factor, factor], axis=1) + mixed
        acc[span] = mixed.reshape(count, rows, 2 * head)
        top[span] = high.reshape(count, rows, head)

    def set_bias(b, first):
        allowed = jnp.concatenate([segcol[...]] * (rows // head), axis=1) == segs[b]
        if first:
            r = lax.broadcasted_iota(jnp.int32, (rows, rows), 0)
            c = lax.broadcasted_iota(jnp.int32, (rows, rows), 1)
            allowed = allowed & (c <= r)
        bias[b] = jnp.where(allowed, 0.0, NEG)

    def unit(values):
        code = pick(values)
        b, g = code % 8, code // 8 % 2

        @pl.when(code // 32 == 1)
        def _():
            set_bias(b, False)

        @pl.when(code // 16 % 2 == 1)
        def _():
            several(b, g, range(per_group), False)

    per_send = per_group // 2
    width = per_send * head
    pieces = per_group // per_send

    def o_copy(c, e):
        col = pl.multiple_of((mt * groups * pieces + c) * width, width)
        to = (mt + e) % tp
        return pltpu.make_async_remote_copy(
            src_ref=o_buf.at[pl.ds(pl.multiple_of(to * out_rows, out_rows), out_rows), pl.ds(c * width, width)],
            dst_ref=out_ref.at[:, pl.ds(col, width)],
            send_sem=o_send.at[c * tp + e],
            recv_sem=o_recv.at[c * tp + e],
            device_id={"ctx": me, "tp": to},
            device_id_type=MESH,
        )

    def last_unit(values, g):
        code = pick(values)
        b = code % 8
        live = code // 16 % 2 == 1

        @pl.when(code // 32 == 1)
        def _():
            set_bias(b, False)
        for p in range(pieces):
            @pl.when(live)
            def _():
                several(b, g, range(p * per_send, (p + 1) * per_send), False)
            c = g * pieces + p
            for h in range(per_send):
                i = g * per_group + p * per_send + h
                o_buf[:, i * head:(i + 1) * head] = (acc[i, :, :head] / acc[i, :, head:]).astype(jnp.bfloat16)
            for e in range(1, tp):
                o_copy(c, e).start()
            mine = pl.ds(pl.multiple_of(mt * out_rows, out_rows), out_rows)
            col = pl.multiple_of((mt * groups * pieces + c) * width, width)
            out_ref[:, pl.ds(col, width)] = o_buf[mine, c * width:(c + 1) * width]

    for slot in EVENTS[0]:
        event(slot)
    q_load.wait()
    segcol[...] = jnp.transpose(jnp.broadcast_to(segs[me], (head, rows)))
    set_bias(me, True)
    for step, values in enumerate(UNITS):
        if step > 0:
            for slot in EVENTS[step]:
                event(slot)
        if step < groups:
            for h in range(step * per_group, (step + 1) * per_group):
                q_ref[h] = q_raw[:, h, :]
            several(me, step, range(per_group), True)
        elif step in LAST:
            last_unit(values, LAST.index(step))
        else:
            unit(values)
    for slot in EVENTS[len(UNITS)]:
        event(slot)

    for group in EVENTS:
        for slot in group:
            drain(slot)
    for c in range(groups * pieces):
        for e in range(1, tp):
            o_copy(c, e).wait()


def planned(queries, keys, values, segment_ids):
    rows, heads, head = queries.shape
    groups = keys.shape[1]
    per_group = heads // groups
    n = lax.axis_size("ctx")
    tp = lax.axis_size("tp")
    chunks = groups * 2
    hbm = pl.BlockSpec(memory_space=pltpu.HBM)
    dma = pltpu.SemaphoreType.DMA
    cfg = (n, tp, groups, per_group, rows, head)
    return pl.pallas_call(
        functools.partial(planned_kernel, cfg),
        out_shape=pltpu.VMEM((rows // tp, tp * heads * head), jnp.bfloat16),
        in_specs=[hbm] * 4,
        out_specs=pl.BlockSpec(memory_space=pltpu.VMEM),
        scratch_shapes=[
            pltpu.VMEM((rows, heads, head), jnp.bfloat16),
            pltpu.VMEM((2, rows, groups, head), jnp.bfloat16),
            pltpu.VMEM((heads, rows, head), jnp.bfloat16),
            pltpu.VMEM((n, groups, 2, rows, head), jnp.bfloat16),
            pltpu.VMEM((n, 1, rows), jnp.int32),
            pltpu.VMEM((rows, head), jnp.int32),
            pltpu.VMEM((n, rows, rows), jnp.float32),
            pltpu.VMEM((heads, rows, 2 * head), jnp.float32),
            pltpu.VMEM((heads, rows, head), jnp.float32),
            pltpu.VMEM((rows, heads * head), jnp.bfloat16),
            dma((4,)),
            dma((n * groups * 2 * 3,)),
            dma((n * groups * 2,)),
            dma((n * 3,)),
            dma((n,)),
            dma((chunks * tp,)),
            dma((chunks * tp,)),
        ],
        compiler_params=pltpu.CompilerParams(
            collective_id=0, has_side_effects=True, vmem_limit_bytes=56 * 1024 * 1024
        ),
    )(queries, keys, values, segment_ids.reshape(1, rows))


def fits_plan(mesh):
    n = mesh.shape["ctx"]
    return plane_width(mesh) == 2 and n == len(UNITS[0])


def solution(mesh):
    in_specs = (P("ctx", "tp", None), P("ctx", "tp", None), P("ctx", "tp", None), P("ctx"))
    out_specs = P(("ctx", "tp"), None)
    body = planned if fits_plan(mesh) else functools.partial(local, plane_width(mesh))
    return jax.shard_map(body, mesh=mesh, in_specs=in_specs, out_specs=out_specs, check_vma=False)
```
